64 devices in a mesh: rep: 4 (over x, y), dp: 16 (over z, core).
Axes of the slice: x: 2, y: 2, z: 8, core: 2. Of those that a mesh axis runs over, the one named last changes fastest.
The devices are a block of a 4x4x8 slice.
Arguments:
- x: bfloat16 [64, 4096, 640], P(('rep', 'dp')), parts along dimension 0
- dy: bfloat16 [64, 4096, 640], P(('rep', 'dp')), parts along dimension 0
- w_gate: bfloat16 [2, 640, 1536], P(None, 'dp')
- w_up: bfloat16 [2, 640, 1536], P(None, 'dp')
- w_down: bfloat16 [2, 1536, 640], P(None, 'dp')
- m_w_gate: float32 [2, 640, 1536], P(None, 'dp')
- m_w_up: float32 [2, 640, 1536], P(None, 'dp')
- m_w_down: float32 [2, 1536, 640], P(None, 'dp')
- v_w_gate: float32 [2, 640, 1536], P(None, 'dp')
- v_w_up: float32 [2, 640, 1536], P(None, 'dp')
- v_w_down: float32 [2, 1536, 640], P(None, 'dp')
Outputs:
- output 1: bfloat16 [8, 640, 1536], P('rep', 'dp'), parts along dimension 0
- output 2: bfloat16 [8, 640, 1536], P('rep', 'dp'), parts along dimension 0
- output 3: bfloat16 [8, 1536, 640], P('rep', 'dp'), parts along dimension 0
- output 4: float32 [8, 640, 1536], P('rep', 'dp'), parts along dimension 0
- output 5: float32 [8, 640, 1536], P('rep', 'dp'), parts along dimension 0
- output 6: float32 [8, 1536, 640], P('rep', 'dp'), parts along dimension 0
- output 7: float32 [8, 640, 1536], P('rep', 'dp'), parts along dimension 0
- output 8: float32 [8, 640, 1536], P('rep', 'dp'), parts along dimension 0
- output 9: float32 [8, 1536, 640], P('rep', 'dp'), parts along dimension 0
There are 4 independent parts. The reference program is written for one: setup_inputs(seed, part) draws one part's arguments, and reference() takes and returns one part's arrays. A program takes and returns all parts, laid end to end along the dimension named above; an argument that names none is the same for every part.
All inputs are finite; a program needn't handle non-finite values.
Results may differ from the reference program's by a relative error of at most 0.0221.
Values are sent between devices in bfloat16 or wider.
A program may use at most 768 MiB of HBM per device.

```python
import jax
import jax.numpy as jnp
from jax import lax

SEQUENCES = 16
TOKENS = 4096
D = 640
FF = 1536
LAYERS = 2
NAMES = ("w_gate", "w_up", "w_down")
SHAPES = {"w_gate": (LAYERS, D, FF), "w_up": (LAYERS, D, FF), "w_down": (LAYERS, FF, D)}


def bump(key, n, height):
    away = (jnp.arange(n, dtype=jnp.int32) - jax.random.randint(key, (), 0, n, jnp.int32)) % n
    return jnp.where(away < n // 8, height, 1.0)


def together(key, own, strength):
    shared = jax.random.normal(key, own.shape[1:], jnp.float32)
    return (own + strength * shared) * lax.rsqrt(1 + strength * strength)


def setup_inputs(seed: int = 0, part: int = 0) -> dict:
    kx, kdy, ka, kb, kz, kf, kh, kl, *keys = jax.random.split(jax.random.key(seed), 8 + 3 * len(NAMES))
    kx, kdy, ka, kb = (jax.random.fold_in(k, part) for k in (kx, kdy, ka, kb))
    kw, km, kv = (keys[i::3] for i in range(3))
    shape = (SEQUENCES, TOKENS, D)
    much_x, much_dy = jax.random.uniform(kz, (2,), jnp.float32, 0.0, 1.0)
    loud = 2.0 ** jax.random.uniform(jax.random.fold_in(kz, 1), (), jnp.float32, -1.0, 2.0)
    layers = 2.0 ** jax.random.uniform(kl, (LAYERS, 1, 1), jnp.float32, -1.0, 1.0)
    x = together(ka, jax.random.normal(kx, shape, jnp.float32), much_x) * bump(kf, D, 4.0)
    dy = together(kb, jax.random.normal(kdy, shape, jnp.float32), much_dy)
    drawn = {"x": x.astype(jnp.bfloat16), "dy": (loud * dy * (SEQUENCES * TOKENS) ** -0.5).astype(jnp.bfloat16)}
    for key, name in zip(kw, NAMES, strict=True):
        w = jax.random.normal(key, SHAPES[name], jnp.float32) * SHAPES[name][1] ** -0.5
        drawn[name] = (w * {"w_gate": 1.0, "w_up": bump(kh, FF, 4.0), "w_down": layers}[name]).astype(jnp.bfloat16)
    for key, name in zip(km, NAMES, strict=True):
        drawn[f"m_{name}"] = 0.1 * jax.random.normal(key, SHAPES[name], jnp.float32)
    for key, name in zip(kv, NAMES, strict=True):
        drawn[f"v_{name}"] = jax.random.uniform(key, SHAPES[name], jnp.float32, 0.005, 0.015)
    return drawn


def matmul(a, w):
    return jnp.dot(a, w, preferred_element_type=jnp.float32).astype(jnp.bfloat16)


def normed(h):
    wide = h.astype(jnp.float32)
    scale = lax.rsqrt(jnp.mean(wide**2, -1, keepdims=True) + 1e-6)
    return (wide * scale).astype(jnp.bfloat16)


def layer(h, w):
    a = normed(h)
    gate = jnp.dot(a, w["w_gate"], preferred_element_type=jnp.float32)
    up = jnp.dot(a, w["w_up"], preferred_element_type=jnp.float32)
    return h + matmul((jax.nn.silu(gate) * up).astype(jnp.bfloat16), w["w_down"])


def adamw(w, m, v, g):
    m = 0.9 * m + 0.1 * g
    v = 0.95 * v + 0.05 * g * g
    step = m * lax.rsqrt(v + 1e-8) + 0.1 * w
    return (w - 0.02 * step).astype(jnp.bfloat16), m, v


def clipped(gradients, sum_of_squares, count):
    factor = jnp.minimum(1.0, 0.5 * lax.rsqrt(sum_of_squares / count + 1e-30))
    return [g * factor for g in gradients]


def stack(weights, h):
    return lax.scan(lambda h, w: (layer(h, w), None), h, weights)[0]


def reference(x, dy, w_gate, w_up, w_down, m_w_gate, m_w_up, m_w_down, v_w_gate, v_w_up, v_w_down):
    weights = dict(zip(NAMES, (w_gate, w_up, w_down), strict=True))

    def take(so_far, sequence):
        h, by_y = sequence
        _, back = jax.vjp(lambda w: stack(w, h), weights)
        return jax.tree.map(lambda total, term: total + term.astype(jnp.float32), so_far, back(by_y)[0]), None

    none_yet = {name: jnp.zeros(w.shape, jnp.float32) for name, w in weights.items()}
    by_weights, _ = lax.scan(take, none_yet, (x, dy))
    gradients = [by_weights[name].astype(jnp.bfloat16).astype(jnp.float32) for name in NAMES]
    gradients = clipped(gradients, sum(jnp.sum(g * g) for g in gradients), sum(g.size for g in gradients))
    new = [
        adamw(w.astype(jnp.float32), m, v, g)
        for w, m, v, g in zip((w_gate, w_up, w_down), (m_w_gate, m_w_up, m_w_down), (v_w_gate, v_w_up, v_w_down), gradients, strict=True)
    ]
    return tuple(one[which] for which in range(3) for one in new)
```

```python
import functools

import jax
import jax.numpy as jnp
from jax import lax
from jax.experimental import pallas as pl
from jax.experimental.pallas import tpu as pltpu
from jax.sharding import PartitionSpec as P

MESH = pl.DeviceIdType.MESH
BF, F32 = jnp.bfloat16, jnp.float32
ANY = pl.BlockSpec(memory_space=pl.ANY)
VM = pl.BlockSpec(memory_space=pltpu.VMEM)
TILE = 512
COLS = 512
LIMIT = 60 * 1024 * 1024


def dot(a, b, ca=1, cb=0):
    return lax.dot_general(a, b, (((ca,), (cb,)), ((), ())), preferred_element_type=F32)


def rounded(a):
    return a.astype(BF).astype(F32)


def norm_of(h):
    wide = h.astype(F32)
    scale = lax.rsqrt(jnp.mean(wide * wide, -1, keepdims=True) + 1e-6)
    return wide, scale, (wide * scale).astype(BF)


def place():
    me = lax.axis_index("dp")
    z, c = me // 2, me % 2
    return z, c, lambda zz, cc: {"dp": zz * 2 + cc}


def greet(peers):
    barrier = pltpu.get_barrier_semaphore()
    for p in peers:
        pl.semaphore_signal(barrier, inc=1, device_id=p, device_id_type=MESH)
    pl.semaphore_wait(barrier, len(peers))


def reach(m, chips):
    far, near = chips // 2, chips - 1 - chips // 2
    return (far, near) if m % 2 == 0 else (near, far)


class Gather:
    def __init__(self, chips, m, src, out, sems):
        self.chips, self.m, self.src, self.out = chips, m, src, out
        self.ring_s, self.ring_r, self.side_s, self.side_r, self.own = sems
        self.rows = src.shape[0]
        self.z, self.c, self.dev = place()
        self.hops = reach(m, chips)
        self.sent = []

    def at(self, zz, cc):
        return self.out.at[pl.ds(pl.multiple_of((zz * 2 + cc) * self.rows, 8), self.rows)]

    def ring(self, way, k, src=None):
        step = 1 if way == 0 else -1
        origin = (self.z - step * k + self.chips) % self.chips
        to = (self.z + step + self.chips) % self.chips
        block = self.at(origin, self.c)
        i = (0 if way == 0 else self.hops[0]) + k
        return pltpu.make_async_remote_copy(
            src_ref=block if src is None else src, dst_ref=block, send_sem=self.ring_s.at[self.m, i], recv_sem=self.ring_r.at[self.m, i],
            device_id=self.dev(to, self.c), device_id_type=MESH)

    def side(self, origin, i, src=None):
        block = self.at(origin, self.c)
        return pltpu.make_async_remote_copy(
            src_ref=block if src is None else src, dst_ref=block, send_sem=self.side_s.at[self.m, i], recv_sem=self.side_r.at[self.m, i],
            device_id=self.dev(self.z, 1 - self.c), device_id_type=MESH)

    def start(self):
        for way in (0, 1):
            self.sent.append(self.ring(way, 0, self.src))
            self.sent[-1].start()
        self.sent.append(self.side(self.z, 0, self.src))
        self.sent[-1].start()
        self.local = pltpu.make_async_copy(self.src, self.at(self.z, self.c), self.own.at[self.m])
        self.local.start()

    def step(self, k):
        for way in (0, 1):
            if k > self.hops[way]:
                continue
            self.ring(way, k - 1).wait_recv()
            if k < self.hops[way]:
                self.sent.append(self.ring(way, k))
                self.sent[-1].start()
            origin = (self.z - (1 if way == 0 else -1) * k + self.chips) % self.chips
            self.sent.append(self.side(origin, k + (0 if way == 0 else self.hops[0])))
            self.sent[-1].start()

    def finish(self):
        for copy in self.sent:
            copy.wait_send()
        for i in range(self.chips):
            self.side(self.z, i).wait_recv()
        self.local.wait()


def gather_sems(n, chips):
    return [pltpu.SemaphoreType.DMA((n, chips - 1))] * 2 + [pltpu.SemaphoreType.DMA((n, chips))] * 2 + [pltpu.SemaphoreType.DMA((n,))]


def gather_kernel(chips, layers, *refs):
    shards, outs, sems = refs[:3], refs[3 : 3 + 3 * layers], refs[3 + 3 * layers :]
    z, c, dev = place()
    greet([dev((z + 1) % chips, c), dev((z + chips - 1) % chips, c), dev(z, 1 - c)])
    all_of = [Gather(chips, l * 3 + i, shards[i].at[l], outs[l * 3 + i], sems) for l in range(layers) for i in range(3)]
    for one in all_of:
        one.start()
    for k in range(1, chips // 2 + 1):
        for one in all_of:
            one.step(k)
    for one in all_of:
        one.finish()


def gather_all(weights, n):
    layers = weights[0].shape[0]
    chips = n // 2
    return pl.pallas_call(
        functools.partial(gather_kernel, chips, layers),
        out_shape=[jax.ShapeDtypeStruct((w.shape[1] * n, w.shape[2]), w.dtype) for _ in range(layers) for w in weights],
        in_specs=[VM] * 3,
        out_specs=[ANY] * (3 * layers),
        scratch_shapes=gather_sems(3 * layers, chips),
        compiler_params=pltpu.CompilerParams(collective_id=0, has_side_effects=True),
        name="gather",
    )(*weights)


class Scatter:
    def __init__(self, chips, l, grads, own, side, slots, sems):
        self.chips, self.l, self.grads, self.own, self.sides, self.slots = chips, l, grads, own, side, slots
        self.own_sem, self.side_s, self.side_r, self.ring_s, self.ring_r = sems
        self.z, self.c, self.dev = place()
        self.sent = []

    def part(self, i, zz, cc):
        rows = self.own[i].shape[-2]
        return self.grads[i].at[pl.ds(pl.multiple_of((zz * 2 + cc) * rows, 8), rows)]

    def chunk(self, way, k):
        return (self.z - 1 - k + 2 * self.chips) % self.chips if way == 0 else (self.z + 1 + k) % self.chips

    def local(self, i, zz):
        return pltpu.make_async_copy(self.part(i, zz, self.c), self.own[i].at[self.l, zz], self.own_sem.at[self.l, i, zz])

    def side(self, i, zz):
        return pltpu.make_async_remote_copy(
            src_ref=self.part(i, zz, 1 - self.c), dst_ref=self.sides[i].at[self.l, zz], send_sem=self.side_s.at[self.l, i, zz],
            recv_sem=self.side_r.at[self.l, i, zz], device_id=self.dev(self.z, 1 - self.c), device_id_type=MESH)

    def start(self):
        for k in range(self.chips):
            away = 0 if k == self.chips - 1 else -1 - k // 2 if k % 2 == 0 else 1 + k // 2
            for i, zz in ((0, self.chunk(0, k)), (1, self.chunk(1, k)), (2, (self.z + self.chips + away) % self.chips)):
                self.side(i, zz).start()
                self.local(i, zz).start()

    def ready(self, i, zz):
        self.local(i, zz).wait()
        self.side(i, zz).wait()

    def ring(self, way, j, k):
        ref = self.slots[way * 2 + j]
        to = (self.z + (1 if way == 0 else self.chips - 1)) % self.chips
        return pltpu.make_async_remote_copy(
            src_ref=ref.at[self.l, k], dst_ref=ref.at[self.l, k + 1], send_sem=self.ring_s.at[self.l, way * 2 + j, k],
            recv_sem=self.ring_r.at[self.l, way * 2 + j, k], device_id=self.dev(to, self.c), device_id_type=MESH)

    def step(self, k):
        for way in (0, 1):
            zz = self.chunk(way, k)
            for j in (0, 1):
                i = way if j == 0 else 2
                ref = self.slots[way * 2 + j]
                if j == 0:
                    self.ready(i, zz)
                    terms = self.own[i][self.l, zz].astype(F32) + self.sides[i][self.l, zz].astype(F32)
                else:
                    if 2 * k < self.chips - 1 if way == 0 else 2 * k < self.chips - 2:
                        self.ready(i, zz)
                    elif way == 0 and k == self.chips - 1:
                        self.ready(i, zz)
                    half = self.own[i].shape[-2] // 2
                    rows = pl.ds(way * half, half)
                    terms = self.own[i][self.l, zz, rows].astype(F32) + self.sides[i][self.l, zz, rows].astype(F32)
                if k > 0:
                    self.ring(way, j, k - 1).wait_recv()
                    terms = terms + ref[self.l, k].astype(F32)
                ref[self.l, k] = terms.astype(BF)
                if k < self.chips - 1:
                    self.ring(way, j, k).start()

    def finish(self):
        for way in (0, 1):
            for j in (0, 1):
                for k in range(self.chips - 1):
                    self.ring(way, j, k).wait_send()


def scatter_kernel(chips, layers, *refs):
    n = 3 * layers
    grads, outs, total = refs[:n], refs[n : n + 3], refs[n + 3]
    own, side, slots, mine, sems = refs[n + 4 : n + 7], refs[n + 7 : n + 10], refs[n + 10 : n + 14], refs[n + 14], refs[n + 15 : n + 20]
    sq_s, sq_r, pair, pair_sem = refs[n + 20 : n + 24]
    z, c, dev = place()
    others = [(z + k) % chips for k in range(1, chips)]
    greet([dev(o, c) for o in others] + [dev(z, 1 - c)])
    all_of = [Scatter(chips, l, grads[3 * l : 3 * l + 3], own, side, slots, sems) for l in reversed(range(layers))]
    for one in all_of:
        one.start()
    for k in range(chips):
        for one in all_of:
            one.step(k)
    squares = jnp.zeros((), F32)
    for l in range(layers):
        half = outs[2].shape[1] // 2
        for ref, out in ((slots[0], outs[0].at[l]), (slots[2], outs[1].at[l]), (slots[1], outs[2].at[l, :half]), (slots[3], outs[2].at[l, half:])):
            g = ref[l, chips - 1].astype(F32)
            out[...] = g
            squares = squares + jnp.sum(g * g)
    mine[0] = jnp.full(mine.shape[1:], squares, F32)
    copies = [
        pltpu.make_async_remote_copy(src_ref=mine.at[0], dst_ref=mine.at[k], send_sem=sq_s.at[k], recv_sem=sq_r.at[k], device_id=dev(o, c), device_id_type=MESH)
        for k, o in enumerate(others, 1)
    ]
    for copy in copies:
        copy.start()
    for copy in copies:
        copy.wait()
    pair[0] = jnp.sum(mine[...], 0)
    copy = pltpu.make_async_remote_copy(src_ref=pair.at[0], dst_ref=pair.at[1], send_sem=pair_sem.at[0], recv_sem=pair_sem.at[1], device_id=dev(z, 1 - c), device_id_type=MESH)
    copy.start()
    copy.wait()
    total[...] = pair[0] + pair[1]
    for one in all_of:
        one.finish()


def scatter_all(grads, n):
    layers, chips = len(grads) // 3, n // 2
    shapes = [(g.shape[0] // n, g.shape[1]) for g in grads[:3]]
    half = (shapes[2][0] // 2, shapes[2][1])
    sem = pltpu.SemaphoreType.DMA
    scratch = [pltpu.VMEM((layers, chips, *s), BF) for s in shapes] * 2
    scratch += [pltpu.VMEM((layers, chips, *s), BF) for s in (shapes[0], half, shapes[1], half)]
    scratch += [pltpu.VMEM((chips, 8, 128), F32)]
    scratch += [sem((layers, 3, chips))] * 3 + [sem((layers, 4, chips - 1))] * 2
    scratch += [sem((chips,))] * 2 + [pltpu.VMEM((2, 8, 128), F32), sem((2,))]
    return pl.pallas_call(
        functools.partial(scatter_kernel, chips, layers),
        out_shape=[jax.ShapeDtypeStruct((layers, *s), F32) for s in shapes] + [jax.ShapeDtypeStruct((8, 128), F32)],
        in_specs=[ANY] * (3 * layers),
        out_specs=[VM] * 4,
        scratch_shapes=scratch,
        compiler_params=pltpu.CompilerParams(collective_id=1, has_side_effects=True, vmem_limit_bytes=LIMIT),
        name="scatter",
    )(*grads)


def blocks(width):
    return [slice(i, i + COLS) for i in range(0, width, COLS)]


def forward_kernel(x_ref, wg, wu, wd, gate_ref, up_ref, h_ref):
    x = x_ref[0]
    _, _, a = norm_of(x)
    down = jnp.zeros(x.shape, F32)
    for cols in blocks(wg.shape[1]):
        gate, up = dot(a, wg[:, cols]), dot(a, wu[:, cols])
        gate_ref[:, cols], up_ref[:, cols] = gate, up
        act = (gate * jax.nn.sigmoid(gate) * up).astype(BF)
        down += dot(act, wd[cols, :])
    h_ref[0] = (x.astype(F32) + rounded(down)).astype(BF)


def add_to(acc, cols, value):
    @pl.when(pl.program_id(0) == 0)
    def _():
        acc[:, cols] = value

    @pl.when(pl.program_id(0) > 0)
    def _():
        acc[:, cols] += value


def gates_back(gate, up, by_act):
    sig = jax.nn.sigmoid(gate)
    silu = gate * sig
    act = (silu * up).astype(BF)
    by_up = (by_act * silu).astype(BF)
    by_gate = (by_act * up * (sig * (1.0 + gate * (1.0 - sig)))).astype(BF)
    return act, by_gate, by_up


def write_out(accs, outs):
    @pl.when(pl.program_id(0) == pl.num_programs(0) - 1)
    def _():
        outs[0][...] = accs[0][...].astype(BF)
        outs[1][...] = accs[1][...].astype(BF)
        outs[2][...] = accs[2][...].T.astype(BF)


def zero(accs):
    @pl.when(pl.program_id(0) == 0)
    def _():
        for acc in accs:
            acc[...] = jnp.zeros_like(acc)


def top_kernel(h_ref, dy_ref, wg, wu, wd, by_h_ref, og, ou, od, ag, au, ad):
    zero((ag, au, ad))
    by_y = dy_ref[0]
    wide, scale, a = norm_of(h_ref[0])
    a_t, by_y_t = a.T, by_y.T
    by_a_g, by_a_u = jnp.zeros(a.shape, F32), jnp.zeros(a.shape, F32)
    for cols in blocks(wg.shape[1]):
        gate, up = dot(a, wg[:, cols]), dot(a, wu[:, cols])
        by_act = rounded(dot(by_y, wd[cols, :], 1, 1))
        act, by_gate, by_up = gates_back(gate, up, by_act)
        ag[:, cols] += dot(a_t, by_gate)
        au[:, cols] += dot(a_t, by_up)
        ad[:, cols] += dot(by_y_t, act)
        by_a_g += dot(by_gate, wg[:, cols], 1, 1)
        by_a_u += dot(by_up, wu[:, cols], 1, 1)
    by_a = rounded(rounded(by_a_g) + rounded(by_a_u))
    by_scale = jnp.sum(by_a * wide, -1, keepdims=True)
    by_h = by_a * scale - wide * (by_scale * scale * scale * scale / wide.shape[-1])
    by_h_ref[0] = (by_y.astype(F32) + rounded(by_h)).astype(BF)
    write_out((ag, au, ad), (og, ou, od))


def bottom_kernel(x_ref, by_y_ref, gate_ref, up_ref, wd, og, ou, od, ag, au, ad):
    zero((ag, au, ad))
    by_y = by_y_ref[0]
    _, _, a = norm_of(x_ref[0])
    a_t, by_y_t = a.T, by_y.T
    for cols in blocks(gate_ref.shape[1]):
        by_act = rounded(dot(by_y, wd[cols, :], 1, 1))
        act, by_gate, by_up = gates_back(gate_ref[:, cols], up_ref[:, cols], by_act)
        ag[:, cols] += dot(a_t, by_gate)
        au[:, cols] += dot(a_t, by_up)
        ad[:, cols] += dot(by_y_t, act)
    write_out((ag, au, ad), (og, ou, od))


def tiles(width):
    return pl.BlockSpec((TILE, width), lambda t: (t, 0))


def states(width):
    return pl.BlockSpec((1, TILE, width), lambda t: (0, t, 0))


def whole(shape):
    return pl.BlockSpec(shape, lambda t: (0, 0), pipeline_mode=pl.Buffered(1))


def local_call(body, grid, in_specs, out_specs, out_shape, scratch, flops, name):
    return pl.pallas_call(
        body, grid=(grid,), in_specs=in_specs, out_specs=out_specs, out_shape=out_shape, scratch_shapes=scratch,
        cost_estimate=pl.CostEstimate(flops=flops, bytes_accessed=flops // 1000, transcendentals=0),
        compiler_params=pltpu.CompilerParams(dimension_semantics=("arbitrary",), vmem_limit_bytes=LIMIT), name=name)


def adamw(w, m, v, g):
    m = 0.9 * m + 0.1 * g
    v = 0.95 * v + 0.05 * g * g
    step = m * lax.rsqrt(v + 1e-8) + 0.1 * w
    return (w - 0.02 * step).astype(BF), m, v


def solution(mesh):
    n = mesh.shape["dp"]

    def step(x, dy, *arrays):
        weights, m, v = (arrays[i : i + 3] for i in (0, 3, 6))
        tokens, d = x.shape[1:]
        ff = weights[0].shape[2]
        grid = tokens // TILE
        flops = 2 * tokens * d * ff
        wg0, wu0, wd0, wg1, wu1, wd1 = gather_all(weights, n)
        state = jax.ShapeDtypeStruct(x.shape, BF)
        wide = jax.ShapeDtypeStruct((tokens, ff), F32)
        across, up_and_down = (d, ff), (ff, d)
        grads = [jax.ShapeDtypeStruct(s, BF) for s in (across, across, up_and_down)]
        accs = [pltpu.VMEM(across, F32)] * 3
        ws = [whole(across), whole(across), whole(up_and_down)]
        gate, up, h = local_call(
            forward_kernel, grid, [states(d)] + ws, [tiles(ff), tiles(ff), states(d)], [wide, wide, state], [], 3 * flops, "forward"
        )(x, wg0, wu0, wd0)
        by_h, *top = local_call(
            top_kernel, grid, [states(d), states(d)] + ws, [states(d)] + ws, [state] + grads, accs, 8 * flops, "top"
        )(h, dy, wg1, wu1, wd1)
        bottom = local_call(
            bottom_kernel, grid, [states(d), states(d), tiles(ff), tiles(ff), ws[2]], ws, grads, accs, 4 * flops, "bottom"
        )(x, by_h, gate, up, wd0)
        *mine, squares = scatter_all(list(bottom) + list(top), n)
        count = n * sum(g.size for g in mine)
        factor = jnp.minimum(1.0, 0.5 * lax.rsqrt(squares[0, 0] / count + 1e-30))
        new = [adamw(w.astype(F32), m, v, g * factor) for w, m, v, g in zip(weights, m, v, mine, strict=True)]
        return tuple(one[which] for which in range(3) for one in new)

    states_spec, cut = P(("rep", "dp"), None, None), P(None, "dp", None)
    return jax.shard_map(
        step,
        mesh=mesh,
        in_specs=(states_spec, states_spec) + (cut,) * 9,
        out_specs=(P("rep", "dp", None),) * 9,
        check_vma=False,
    )
```

```python
import functools

import jax
import jax.numpy as jnp
from jax import lax
from jax.experimental import pallas as pl
from jax.experimental.pallas import tpu as pltpu
from jax.sharding import PartitionSpec as P

MESH = pl.DeviceIdType.MESH
BF, F32 = jnp.bfloat16, jnp.float32
ANY = pl.BlockSpec(memory_space=pl.ANY)
VM = pl.BlockSpec(memory_space=pltpu.VMEM)
TILE = 512
COLS = 512
LIMIT = 60 * 1024 * 1024
MOVES = (0, 1, 2, 4, 6, 8, 9, 11)


def dot(a, b, ca=1, cb=0):
    return lax.dot_general(a, b, (((ca,), (cb,)), ((), ())), preferred_element_type=F32)


def rounded(a):
    return a.astype(BF).astype(F32)


def norm_of(h):
    wide = h.astype(F32)
    scale = lax.rsqrt(jnp.mean(wide * wide, -1, keepdims=True) + 1e-6)
    return wide, scale, (wide * scale).astype(BF)


def place():
    me = lax.axis_index("dp")
    z, c = me // 2, me % 2
    return z, c, lambda zz, cc: {"dp": zz * 2 + cc}


def greet(peers):
    barrier = pltpu.get_barrier_semaphore()
    for p in peers:
        pl.semaphore_signal(barrier, inc=1, device_id=p, device_id_type=MESH)
    pl.semaphore_wait(barrier, len(peers))


def reach(m, chips):
    far, near = chips // 2, chips - 1 - chips // 2
    return (far, near) if m % 2 == 0 else (near, far)


class Gather:
    def __init__(self, chips, m, hops, src, out, sems):
        self.chips, self.m, self.hops, self.src, self.out = chips, m, hops, src, out
        self.ring_s, self.ring_r, self.side_s, self.side_r, self.own = sems
        self.rows = src.shape[0]
        self.z, self.c, self.dev = place()

    def at(self, zz, cc):
        return self.out.at[pl.ds(pl.multiple_of((zz * 2 + cc) * self.rows, 8), self.rows)]

    def ring(self, way, k, src=None):
        step = 1 if way == 0 else -1
        origin = (self.z - step * k + self.chips) % self.chips
        to = (self.z + step + self.chips) % self.chips
        block = self.at(origin, self.c)
        i = (0 if way == 0 else self.hops[0]) + k
        return pltpu.make_async_remote_copy(
            src_ref=block if src is None else src, dst_ref=block, send_sem=self.ring_s.at[self.m, i], recv_sem=self.ring_r.at[self.m, i],
            device_id=self.dev(to, self.c), device_id_type=MESH)

    def side(self, origin, i, src=None):
        block = self.at(origin, self.c)
        return pltpu.make_async_remote_copy(
            src_ref=block if src is None else src, dst_ref=block, send_sem=self.side_s.at[self.m, i], recv_sem=self.side_r.at[self.m, i],
            device_id=self.dev(self.z, 1 - self.c), device_id_type=MESH)

    def keep(self):
        return pltpu.make_async_copy(self.src, self.at(self.z, self.c), self.own.at[self.m])

    def start(self):
        for way in (0, 1):
            self.ring(way, 0, self.src).start()
        self.side(self.z, 0, self.src).start()
        self.keep().start()

    def step(self, k):
        for way in (0, 1):
            if k > self.hops[way]:
                continue
            self.ring(way, k - 1).wait_recv()
            if k < self.hops[way]:
                self.ring(way, k).start()
            origin = (self.z - (1 if way == 0 else -1) * k + self.chips) % self.chips
            self.side(origin, k + (0 if way == 0 else self.hops[0])).start()

    def finish(self):
        for way in (0, 1):
            for k in range(self.hops[way]):
                self.ring(way, k).wait_send()
        for i in range(self.chips):
            self.side(self.z, i).wait()
        self.keep().wait()


def gather_sems(n, chips):
    return [pltpu.SemaphoreType.DMA((n, chips - 1))] * 2 + [pltpu.SemaphoreType.DMA((n, chips))] * 2 + [pltpu.SemaphoreType.DMA((n,))]


def gathers(chips, layer, shards, outs, sems):
    z, c, dev = place()
    peers = [dev((z + 1) % chips, c), dev((z + chips - 1) % chips, c), dev(z, 1 - c)]
    return peers, [Gather(chips, i, reach(i + layer, chips), shards[i].at[layer], outs[i], sems) for i in range(3)]


def gather_kernel(chips, *refs):
    peers, all_of = gathers(chips, 0, refs[:3], refs[3:6], refs[6:])
    greet(peers)
    for one in all_of:
        one.start()
    for k in range(1, chips // 2 + 1):
        for one in all_of:
            one.step(k)
    for one in all_of:
        one.finish()


def gathered(weights, n):
    return [jax.ShapeDtypeStruct((w.shape[1] * n, w.shape[2]), w.dtype) for w in weights]


def gather_first(weights, n):
    chips = n // 2
    return pl.pallas_call(
        functools.partial(gather_kernel, chips),
        out_shape=gathered(weights, n),
        in_specs=[VM] * 3,
        out_specs=[ANY] * 3,
        scratch_shapes=gather_sems(3, chips),
        compiler_params=pltpu.CompilerParams(collective_id=0, has_side_effects=True),
        name="gather",
    )(*weights)


class Scatter:
    def __init__(self, chips, grads, scratch):
        self.chips, self.grads = chips, grads
        self.own, self.sides, self.slots = scratch[:3], scratch[3:6], scratch[6:10]
        self.own_sem, self.side_s, self.side_r, self.ring_s, self.ring_r = scratch[10:15]
        self.z, self.c, self.dev = place()
        self.peers = [self.dev((self.z + 1) % chips, self.c), self.dev((self.z + chips - 1) % chips, self.c), self.dev(self.z, 1 - self.c)]

    def part(self, i, zz, cc):
        rows = self.own[i].shape[-2]
        return self.grads[i].at[pl.ds(pl.multiple_of((zz * 2 + cc) * rows, 8), rows)]

    def chunk(self, way, k):
        return (self.z - 1 - k + 2 * self.chips) % self.chips if way == 0 else (self.z + 1 + k) % self.chips

    def local(self, i, zz):
        return pltpu.make_async_copy(self.part(i, zz, self.c), self.own[i].at[zz], self.own_sem.at[i, zz])

    def side(self, i, zz):
        return pltpu.make_async_remote_copy(
            src_ref=self.part(i, zz, 1 - self.c), dst_ref=self.sides[i].at[zz], send_sem=self.side_s.at[i, zz],
            recv_sem=self.side_r.at[i, zz], device_id=self.dev(self.z, 1 - self.c), device_id_type=MESH)

    def start(self):
        for k in range(self.chips):
            away = 0 if k == self.chips - 1 else -1 - k // 2 if k % 2 == 0 else 1 + k // 2
            for i, zz in ((0, self.chunk(0, k)), (1, self.chunk(1, k)), (2, (self.z + self.chips + away) % self.chips)):
                self.side(i, zz).start()
                self.local(i, zz).start()

    def ready(self, i, zz):
        self.local(i, zz).wait()
        self.side(i, zz).wait()

    def ring(self, way, j, k):
        ref = self.slots[way * 2 + j]
        to = (self.z + (1 if way == 0 else self.chips - 1)) % self.chips
        return pltpu.make_async_remote_copy(
            src_ref=ref.at[k], dst_ref=ref.at[k + 1], send_sem=self.ring_s.at[way * 2 + j, k],
            recv_sem=self.ring_r.at[way * 2 + j, k], device_id=self.dev(to, self.c), device_id_type=MESH)

    def step(self, k):
        for way in (0, 1):
            zz = self.chunk(way, k)
            for j in (0, 1):
                i = way if j == 0 else 2
                ref = self.slots[way * 2 + j]
                if j == 0:
                    self.ready(i, zz)
                    terms = self.own[i][zz].astype(F32) + self.sides[i][zz].astype(F32)
                else:
                    if 2 * k < self.chips - 1 if way == 0 else 2 * k < self.chips - 2:
                        self.ready(i, zz)
                    elif way == 0 and k == self.chips - 1:
                        self.ready(i, zz)
                    half = self.own[i].shape[-2] // 2
                    rows = pl.ds(way * half, half)
                    terms = self.own[i][zz, rows].astype(F32) + self.sides[i][zz, rows].astype(F32)
                if k > 0:
                    self.ring(way, j, k - 1).wait_recv()
                    terms = terms + ref[k].astype(F32)
                ref[k] = terms.astype(BF)
                if k < self.chips - 1:
                    self.ring(way, j, k).start()

    def finish(self):
        for way in (0, 1):
            for j in (0, 1):
                for k in range(self.chips - 1):
                    self.ring(way, j, k).wait_send()


    def blocks(self):
        last, half = self.chips - 1, self.own[2].shape[-2] // 2
        return (0, slice(None), self.slots[0][last]), (1, slice(None), self.slots[2][last]), (2, slice(0, half), self.slots[1][last]), (2, slice(half, None), self.slots[3][last])


def block_shapes(grads, n):
    return [(g.shape[0] // n, g.shape[1]) for g in grads]


def scatter_scratch(shapes, chips):
    half = (shapes[2][0] // 2, shapes[2][1])
    sem = pltpu.SemaphoreType.DMA
    scratch = [pltpu.VMEM((chips, *s), BF) for s in shapes] * 2
    scratch += [pltpu.VMEM((chips, *s), BF) for s in (shapes[0], half, shapes[1], half)]
    return scratch + [sem((3, chips))] * 3 + [sem((4, chips - 1))] * 2


def scatter_kernel(chips, *refs):
    grads, done, outs, total = refs[:3], refs[3:6], refs[6:9], refs[9]
    mine, sq_s, sq_r, pair, pair_sem = refs[25:]
    z, c, dev = place()
    others = [(z + k) % chips for k in range(1, chips)]
    greet([dev(o, c) for o in others] + [dev(z, 1 - c)])
    one = Scatter(chips, grads, refs[10:25])
    one.start()
    squares = jnp.zeros((), F32)
    for k in range(chips):
        one.step(k)
        if k < 3:
            g = done[k][...].astype(F32)
            outs[k][1] = g
            squares += jnp.sum(g * g)
    for i, rows, g in one.blocks():
        g = g.astype(F32)
        outs[i][0, rows] = g
        squares += jnp.sum(g * g)
    mine[0] = jnp.full(mine.shape[1:], squares, F32)
    copies = [
        pltpu.make_async_remote_copy(src_ref=mine.at[0], dst_ref=mine.at[k], send_sem=sq_s.at[k], recv_sem=sq_r.at[k], device_id=dev(o, c), device_id_type=MESH)
        for k, o in enumerate(others, 1)
    ]
    for copy in copies:
        copy.start()
    for copy in copies:
        copy.wait()
    pair[0] = jnp.sum(mine[...], 0)
    copy = pltpu.make_async_remote_copy(src_ref=pair.at[0], dst_ref=pair.at[1], send_sem=pair_sem.at[0], recv_sem=pair_sem.at[1], device_id=dev(z, 1 - c), device_id_type=MESH)
    copy.start()
    copy.wait()
    total[...] = pair[0] + pair[1]
    one.finish()


def scatter_last(grads, done, n):
    chips = n // 2
    shapes = block_shapes(grads, n)
    sem = pltpu.SemaphoreType.DMA
    return pl.pallas_call(
        functools.partial(scatter_kernel, chips),
        out_shape=[jax.ShapeDtypeStruct((2, *s), F32) for s in shapes] + [jax.ShapeDtypeStruct((8, 128), F32)],
        in_specs=[ANY] * 3 + [VM] * 3,
        out_specs=[VM] * 4,
        scratch_shapes=scatter_scratch(shapes, chips) + [pltpu.VMEM((chips, 8, 128), F32), sem((chips,)), sem((chips,)), pltpu.VMEM((2, 8, 128), F32), sem((2,))],
        compiler_params=pltpu.CompilerParams(collective_id=1, has_side_effects=True, vmem_limit_bytes=LIMIT),
        name="scatter",
    )(*grads, *done)


def blocks(width):
    return [slice(i, i + COLS) for i in range(0, width, COLS)]


def forward_kernel(chips, x_ref, wg, wu, wd, *refs):
    shards, (gate_ref, up_ref, h_ref), outs, sems = refs[:3], refs[3:6], refs[6:9], refs[9:]
    t, last = pl.program_id(0), pl.num_programs(0) - 1
    peers, all_of = gathers(chips, 1, shards, outs, sems)
    moves = [(one, k) for k in range(1, chips // 2 + 1) for one in all_of]

    @pl.when(t == 0)
    def _():
        greet(peers)
        for one in all_of:
            one.start()

    for at, (begin, end) in enumerate(zip(MOVES, MOVES[1:]), 1):
        @pl.when(t == at)
        def _():
            for one, k in moves[begin:end]:
                one.step(k)

    x = x_ref[0]
    _, _, a = norm_of(x)
    down = jnp.zeros(x.shape, F32)
    for cols in blocks(wg.shape[1]):
        gate, up = dot(a, wg[:, cols]), dot(a, wu[:, cols])
        gate_ref[:, cols], up_ref[:, cols] = gate, up
        act = (gate * jax.nn.sigmoid(gate) * up).astype(BF)
        down += dot(act, wd[cols, :])
    h_ref[0] = (x.astype(F32) + rounded(down)).astype(BF)

    @pl.when(t == last)
    def _():
        for one, k in moves[MOVES[-1]:]:
            one.step(k)
        for one in all_of:
            one.finish()


def gates_back(gate, up, by_act):
    sig = jax.nn.sigmoid(gate)
    silu = gate * sig
    act = (silu * up).astype(BF)
    by_up = (by_act * silu).astype(BF)
    by_gate = (by_act * up * (sig * (1.0 + gate * (1.0 - sig)))).astype(BF)
    return act, by_gate, by_up


def write_out(accs, outs):
    @pl.when(pl.program_id(0) == pl.num_programs(0) - 1)
    def _():
        outs[0][...] = accs[0][...].astype(BF)
        outs[1][...] = accs[1][...].astype(BF)
        outs[2][...] = accs[2][...].T.astype(BF)


def zero(accs):
    @pl.when(pl.program_id(0) == 0)
    def _():
        for acc in accs:
            acc[...] = jnp.zeros_like(acc)


def top_kernel(h_ref, dy_ref, wg, wu, wd, by_h_ref, og, ou, od, ag, au, ad):
    zero((ag, au, ad))
    by_y = dy_ref[0]
    wide, scale, a = norm_of(h_ref[0])
    a_t, by_y_t = a.T, by_y.T
    by_a_g, by_a_u = jnp.zeros(a.shape, F32), jnp.zeros(a.shape, F32)
    for cols in blocks(wg.shape[1]):
        gate, up = dot(a, wg[:, cols]), dot(a, wu[:, cols])
        by_act = rounded(dot(by_y, wd[cols, :], 1, 1))
        act, by_gate, by_up = gates_back(gate, up, by_act)
        ag[:, cols] += dot(a_t, by_gate)
        au[:, cols] += dot(a_t, by_up)
        ad[:, cols] += dot(by_y_t, act)
        by_a_g += dot(by_gate, wg[:, cols], 1, 1)
        by_a_u += dot(by_up, wu[:, cols], 1, 1)
    by_a = rounded(rounded(by_a_g) + rounded(by_a_u))
    by_scale = jnp.sum(by_a * wide, -1, keepdims=True)
    by_h = by_a * scale - wide * (by_scale * scale * scale * scale / wide.shape[-1])
    by_h_ref[0] = (by_y.astype(F32) + rounded(by_h)).astype(BF)
    write_out((ag, au, ad), (og, ou, od))


def bottom_kernel(chips, x_ref, by_y_ref, gate_ref, up_ref, wd, *refs):
    top, (og, ou, od), done, (ag, au, ad) = refs[:3], refs[3:6], refs[6:9], refs[9:12]
    t, last = pl.program_id(0), pl.num_programs(0) - 1
    one = Scatter(chips, top, refs[12:])

    @pl.when(t == 0)
    def _():
        greet(one.peers)
        one.start()

    for k in range(chips - 1):
        @pl.when(t == k + 1)
        def _():
            one.step(k)

    zero((ag, au, ad))
    by_y = by_y_ref[0]
    _, _, a = norm_of(x_ref[0])
    a_t, by_y_t = a.T, by_y.T
    for cols in blocks(gate_ref.shape[1]):
        by_act = rounded(dot(by_y, wd[cols, :], 1, 1))
        act, by_gate, by_up = gates_back(gate_ref[:, cols], up_ref[:, cols], by_act)
        ag[:, cols] += dot(a_t, by_gate)
        au[:, cols] += dot(a_t, by_up)
        ad[:, cols] += dot(by_y_t, act)
    write_out((ag, au, ad), (og, ou, od))

    @pl.when(t == last)
    def _():
        one.step(chips - 1)
        for i, rows, g in one.blocks():
            done[i][rows] = g
        one.finish()


def tiles(width):
    return pl.BlockSpec((TILE, width), lambda t: (t, 0))


def states(width):
    return pl.BlockSpec((1, TILE, width), lambda t: (0, t, 0))


def whole(shape):
    return pl.BlockSpec(shape, lambda t: (0,) * len(shape), pipeline_mode=pl.Buffered(1))


def tiled_call(body, grid, in_specs, out_specs, out_shape, scratch, flops, name, **more):
    return pl.pallas_call(
        body, grid=(grid,), in_specs=in_specs, out_specs=out_specs, out_shape=out_shape, scratch_shapes=scratch,
        cost_estimate=pl.CostEstimate(flops=flops, bytes_accessed=flops // 1000, transcendentals=0),
        compiler_params=pltpu.CompilerParams(dimension_semantics=("arbitrary",), vmem_limit_bytes=LIMIT, **more), name=name)


def adamw(w, m, v, g):
    m = 0.9 * m + 0.1 * g
    v = 0.95 * v + 0.05 * g * g
    step = m * lax.rsqrt(v + 1e-8) + 0.1 * w
    return (w - 0.02 * step).astype(BF), m, v


def solution(mesh):
    n = mesh.shape["dp"]

    def step(x, dy, *arrays):
        weights, m, v = (arrays[i : i + 3] for i in (0, 3, 6))
        tokens, d = x.shape[1:]
        ff = weights[0].shape[2]
        grid = tokens // TILE
        flops = 2 * tokens * d * ff
        chips = n // 2
        assert grid == chips
        wg0, wu0, wd0 = gather_first(weights, n)
        state = jax.ShapeDtypeStruct(x.shape, BF)
        wide = jax.ShapeDtypeStruct((tokens, ff), F32)
        across, up_and_down = (d, ff), (ff, d)
        grads = [jax.ShapeDtypeStruct(s, BF) for s in (across, across, up_and_down)]
        accs = [pltpu.VMEM(across, F32)] * 3
        ws = [whole(across), whole(across), whole(up_and_down)]
        gate, up, h, *next_w = tiled_call(
            functools.partial(forward_kernel, chips), grid, [states(d)] + ws + [whole(w.shape) for w in weights],
            [tiles(ff), tiles(ff), states(d)] + [ANY] * 3, [wide, wide, state] + gathered(weights, n), gather_sems(3, chips), 3 * flops, "forward",
            collective_id=2, has_side_effects=True,
        )(x, wg0, wu0, wd0, *weights)
        by_h, *top = tiled_call(
            top_kernel, grid, [states(d), states(d)] + ws, [states(d)] + ws, [state] + grads, accs, 8 * flops, "top"
        )(h, dy, *next_w)
        shapes = block_shapes(grads, n)
        *bottom, b0, b1, b2 = tiled_call(
            functools.partial(bottom_kernel, chips), grid, [states(d), states(d), tiles(ff), tiles(ff), ws[2]] + [ANY] * 3,
            ws + [whole(b) for b in shapes], grads + [jax.ShapeDtypeStruct(b, BF) for b in shapes],
            accs + scatter_scratch(shapes, chips), 4 * flops, "bottom", collective_id=3, has_side_effects=True,
        )(x, by_h, gate, up, wd0, *top)
        *mine, squares = scatter_last(bottom, (b0, b1, b2), n)
        count = n * sum(g.size for g in mine)
        factor = jnp.minimum(1.0, 0.5 * lax.rsqrt(squares[0, 0] / count + 1e-30))
        new = [adamw(w.astype(F32), m, v, g * factor) for w, m, v, g in zip(weights, m, v, mine, strict=True)]
        return tuple(one[which] for which in range(3) for one in new)

    states_spec, cut = P(("rep", "dp"), None, None), P(None, "dp", None)
    return jax.shard_map(
        step,
        mesh=mesh,
        in_specs=(states_spec, states_spec) + (cut,) * 9,
        out_specs=(P("rep", "dp", None),) * 9,
        check_vma=False,
    )
```

```python
import functools

import jax
import jax.numpy as jnp
from jax import lax
from jax.experimental import pallas as pl
from jax.experimental.pallas import tpu as pltpu
from jax.sharding import PartitionSpec as P

MESH = pl.DeviceIdType.MESH
BF, F32 = jnp.bfloat16, jnp.float32
ANY = pl.BlockSpec(memory_space=pl.ANY)
VM = pl.BlockSpec(memory_space=pltpu.VMEM)
TILE = 512
TILE_FORWARD = 256
COLS = 768
LIMIT = 60 * 1024 * 1024
MOVES = (0, 0, 0, 1, 2, 3, 3, 4, 5, 6, 7, 7, 8, 9, 10, 11)


def dot(a, b, ca=1, cb=0):
    return lax.dot_general(a, b, (((ca,), (cb,)), ((), ())), preferred_element_type=F32)


def rounded(a):
    return a.astype(BF).astype(F32)


def norm_of(h):
    wide = h.astype(F32)
    scale = lax.rsqrt(jnp.mean(wide * wide, -1, keepdims=True) + 1e-6)
    return wide, scale, (wide * scale).astype(BF)


def place():
    me = lax.axis_index("dp")
    z, c = me // 2, me % 2
    return z, c, lambda zz, cc: {"dp": zz * 2 + cc}


def greet(peers):
    barrier = pltpu.get_barrier_semaphore()
    for p in peers:
        pl.semaphore_signal(barrier, inc=1, device_id=p, device_id_type=MESH)
    pl.semaphore_wait(barrier, len(peers))


def reach(m, chips):
    far, near = chips // 2, chips - 1 - chips // 2
    return (far, near) if m % 2 == 0 else (near, far)


class Gather:
    def __init__(self, chips, m, hops, src, out, sems):
        self.chips, self.m, self.hops, self.src, self.out = chips, m, hops, src, out
        self.ring_s, self.ring_r, self.side_s, self.side_r, self.own = sems
        self.rows = src.shape[0]
        self.z, self.c, self.dev = place()

    def at(self, zz, cc):
        return self.out.at[pl.ds(pl.multiple_of((zz * 2 + cc) * self.rows, 8), self.rows)]

    def ring(self, way, k, src=None):
        step = 1 if way == 0 else -1
        origin = (self.z - step * k + self.chips) % self.chips
        to = (self.z + step + self.chips) % self.chips
        block = self.at(origin, self.c)
        i = (0 if way == 0 else self.hops[0]) + k
        return pltpu.make_async_remote_copy(
            src_ref=block if src is None else src, dst_ref=block, send_sem=self.ring_s.at[self.m, i], recv_sem=self.ring_r.at[self.m, i],
            device_id=self.dev(to, self.c), device_id_type=MESH)

    def side(self, origin, i, src=None):
        block = self.at(origin, self.c)
        return pltpu.make_async_remote_copy(
            src_ref=block if src is None else src, dst_ref=block, send_sem=self.side_s.at[self.m, i], recv_sem=self.side_r.at[self.m, i],
            device_id=self.dev(self.z, 1 - self.c), device_id_type=MESH)

    def keep(self):
        return pltpu.make_async_copy(self.src, self.at(self.z, self.c), self.own.at[self.m])

    def start(self):
        for way in (0, 1):
            self.ring(way, 0, self.src).start()
        self.side(self.z, 0, self.src).start()
        self.keep().start()

    def step(self, k):
        for way in (0, 1):
            if k > self.hops[way]:
                continue
            self.ring(way, k - 1).wait_recv()
            if k < self.hops[way]:
                self.ring(way, k).start()
            origin = (self.z - (1 if way == 0 else -1) * k + self.chips) % self.chips
            self.side(origin, k + (0 if way == 0 else self.hops[0])).start()

    def finish(self):
        for way in (0, 1):
            for k in range(self.hops[way]):
                self.ring(way, k).wait_send()
        for i in range(self.chips):
            self.side(self.z, i).wait()
        self.keep().wait()


def gather_sems(n, chips):
    return [pltpu.SemaphoreType.DMA((n, chips - 1))] * 2 + [pltpu.SemaphoreType.DMA((n, chips))] * 2 + [pltpu.SemaphoreType.DMA((n,))]


def gathers(chips, layer, shards, outs, sems):
    z, c, dev = place()
    peers = [dev((z + 1) % chips, c), dev((z + chips - 1) % chips, c), dev(z, 1 - c)]
    return peers, [Gather(chips, i, reach(i + layer, chips), shards[i].at[layer], outs[i], sems) for i in range(3)]


def gather_kernel(chips, *refs):
    peers, all_of = gathers(chips, 0, refs[:3], refs[3:6], refs[6:])
    greet(peers)
    for one in all_of:
        one.start()
    for k in range(1, chips // 2 + 1):
        for one in all_of:
            one.step(k)
    for one in all_of:
        one.finish()


def gathered(weights, n):
    return [jax.ShapeDtypeStruct((w.shape[1] * n, w.shape[2]), w.dtype) for w in weights]


def gather_first(weights, n):
    chips = n // 2
    return pl.pallas_call(
        functools.partial(gather_kernel, chips),
        out_shape=gathered(weights, n),
        in_specs=[VM] * 3,
        out_specs=[ANY] * 3,
        scratch_shapes=gather_sems(3, chips),
        compiler_params=pltpu.CompilerParams(collective_id=0, has_side_effects=True),
        name="gather",
    )(*weights)


class Scatter:
    def __init__(self, chips, grads, scratch):
        self.chips, self.grads = chips, grads
        self.own, self.sides, self.slots = scratch[:3], scratch[3:6], scratch[6:12]
        self.own_sem, self.side_s, self.side_r, self.ring_s, self.ring_r = scratch[12:17]
        self.z, self.c, self.dev = place()
        self.peers = [self.dev((self.z + 1) % chips, self.c), self.dev((self.z + chips - 1) % chips, self.c), self.dev(self.z, 1 - self.c)]

    def part(self, i, zz, cc):
        rows = self.own[i].shape[-2]
        return self.grads[i].at[pl.ds(pl.multiple_of((zz * 2 + cc) * rows, 8), rows)]

    def chunk(self, way, k):
        return (self.z - 1 - k + 2 * self.chips) % self.chips if way == 0 else (self.z + 1 + k) % self.chips

    def local(self, i, zz):
        return pltpu.make_async_copy(self.part(i, zz, self.c), self.own[i].at[zz], self.own_sem.at[i, zz])

    def side(self, i, zz):
        return pltpu.make_async_remote_copy(
            src_ref=self.part(i, zz, 1 - self.c), dst_ref=self.sides[i].at[zz], send_sem=self.side_s.at[i, zz],
            recv_sem=self.side_r.at[i, zz], device_id=self.dev(self.z, 1 - self.c), device_id_type=MESH)

    def start(self):
        for k in range(self.chips):
            away = 0 if k == self.chips - 1 else -1 - k // 2 if k % 2 == 0 else 1 + k // 2
            for i, zz in ((0, self.chunk(0, k)), (1, self.chunk(1, k)), (2, (self.z + self.chips + away) % self.chips)):
                self.side(i, zz).start()
                self.local(i, zz).start()

    def ready(self, i, zz):
        self.local(i, zz).wait()
        self.side(i, zz).wait()

    def pieces(self, way):
        width, height = self.own[way].shape[-1] // 2, self.own[2].shape[-2] // 2
        every = slice(None)
        return (way, every, slice(0, width)), (way, every, slice(width, None)), (2, slice(way * height, way * height + height), every)

    def ring(self, way, j, k):
        ref = self.slots[way * 3 + j]
        to = (self.z + (1 if way == 0 else self.chips - 1)) % self.chips
        return pltpu.make_async_remote_copy(
            src_ref=ref.at[k], dst_ref=ref.at[k + 1], send_sem=self.ring_s.at[way * 3 + j, k],
            recv_sem=self.ring_r.at[way * 3 + j, k], device_id=self.dev(to, self.c), device_id_type=MESH)

    def step(self, k):
        for j in range(3):
            for way in (0, 1):
                zz = self.chunk(way, k)
                i, rows, cols = self.pieces(way)[j]
                first = 2 * k < self.chips - 1 or k == self.chips - 1 if way == 0 else 2 * k < self.chips - 2
                if j == 0 or j == 2 and first:
                    self.ready(i, zz)
                ref = self.slots[way * 3 + j]
                terms = self.own[i][zz, rows, cols].astype(F32) + self.sides[i][zz, rows, cols].astype(F32)
                if k > 0:
                    self.ring(way, j, k - 1).wait_recv()
                    terms = terms + ref[k].astype(F32)
                ref[k] = terms.astype(BF)
                if k < self.chips - 1:
                    self.ring(way, j, k).start()

    def finish(self):
        for way in (0, 1):
            for j in range(3):
                for k in range(self.chips - 1):
                    self.ring(way, j, k).wait_send()

    def blocks(self):
        return [(*piece, self.slots[way * 3 + j][self.chips - 1]) for way in (0, 1) for j, piece in enumerate(self.pieces(way))]


def block_shapes(grads, n):
    return [(g.shape[0] // n, g.shape[1]) for g in grads]


def scatter_scratch(shapes, chips):
    sem = pltpu.SemaphoreType.DMA
    across = [(h, w // 2) for h, w in shapes[:2]]
    down = (shapes[2][0] // 2, shapes[2][1])
    scratch = [pltpu.VMEM((chips, *s), BF) for s in shapes] * 2
    scratch += [pltpu.VMEM((chips, *s), BF) for s in (across[0], across[0], down, across[1], across[1], down)]
    return scratch + [sem((3, chips))] * 3 + [sem((6, chips - 1))] * 2


def scatter_kernel(chips, *refs):
    grads, done, outs, total = refs[:3], refs[3:6], refs[6:9], refs[9]
    mine, sq_s, sq_r, pair, pair_sem = refs[27:]
    z, c, dev = place()
    others = [(z + k) % chips for k in range(1, chips)]
    greet([dev(o, c) for o in others] + [dev(z, 1 - c)])
    one = Scatter(chips, grads, refs[10:27])
    one.start()
    squares = jnp.zeros((), F32)
    for k in range(chips):
        one.step(k)
        if k < 3:
            g = done[k][...].astype(F32)
            outs[k][1] = g
            squares += jnp.sum(g * g)
    for i, rows, cols, g in one.blocks():
        g = g.astype(F32)
        outs[i][0, rows, cols] = g
        squares += jnp.sum(g * g)
    mine[0] = jnp.full(mine.shape[1:], squares, F32)
    copies = [
        pltpu.make_async_remote_copy(src_ref=mine.at[0], dst_ref=mine.at[k], send_sem=sq_s.at[k], recv_sem=sq_r.at[k], device_id=dev(o, c), device_id_type=MESH)
        for k, o in enumerate(others, 1)
    ]
    for copy in copies:
        copy.start()
    for copy in copies:
        copy.wait()
    pair[0] = jnp.sum(mine[...], 0)
    copy = pltpu.make_async_remote_copy(src_ref=pair.at[0], dst_ref=pair.at[1], send_sem=pair_sem.at[0], recv_sem=pair_sem.at[1], device_id=dev(z, 1 - c), device_id_type=MESH)
    copy.start()
    copy.wait()
    total[...] = pair[0] + pair[1]
    one.finish()


def scatter_last(grads, done, n):
    chips = n // 2
    shapes = block_shapes(grads, n)
    sem = pltpu.SemaphoreType.DMA
    return pl.pallas_call(
        functools.partial(scatter_kernel, chips),
        out_shape=[jax.ShapeDtypeStruct((2, *s), F32) for s in shapes] + [jax.ShapeDtypeStruct((8, 128), F32)],
        in_specs=[ANY] * 3 + [VM] * 3,
        out_specs=[VM] * 4,
        scratch_shapes=scatter_scratch(shapes, chips) + [pltpu.VMEM((chips, 8, 128), F32), sem((chips,)), sem((chips,)), pltpu.VMEM((2, 8, 128), F32), sem((2,))],
        compiler_params=pltpu.CompilerParams(collective_id=1, has_side_effects=True, vmem_limit_bytes=LIMIT),
        name="scatter",
    )(*grads, *done)


def blocks(width, cols=None):
    cols = cols or COLS
    return [slice(i, i + cols) for i in range(0, width, cols)]


def forward_kernel(chips, x_ref, wg, wu, wd, *refs):
    shards, (gate_ref, up_ref, h_ref), outs, sems = refs[:3], refs[3:6], refs[6:9], refs[9:]
    t, last = pl.program_id(0), pl.num_programs(0) - 1
    peers, all_of = gathers(chips, 1, shards, outs, sems)
    moves = [(one, k) for k in range(1, chips // 2 + 1) for one in all_of]

    @pl.when(t == 0)
    def _():
        greet(peers)
        for one in all_of:
            one.start()

    for at, (begin, end) in enumerate(zip(MOVES, MOVES[1:]), 1):
        @pl.when(t == at)
        def _():
            for one, k in moves[begin:end]:
                one.step(k)

    x = x_ref[0]
    _, _, a = norm_of(x)
    down = jnp.zeros(x.shape, F32)
    for cols in blocks(wg.shape[1], wg.shape[1]):
        gate, up = dot(a, wg[:, cols]), dot(a, wu[:, cols])
        gate_ref[:, cols], up_ref[:, cols] = gate, up
        act = (gate * jax.nn.sigmoid(gate) * up).astype(BF)
        down += dot(act, wd[cols, :])
    h_ref[0] = (x.astype(F32) + rounded(down)).astype(BF)

    @pl.when(t == last)
    def _():
        for one, k in moves[MOVES[-1]:]:
            one.step(k)
        for one in all_of:
            one.finish()


def gates_back(gate, up, by_act):
    sig = jax.nn.sigmoid(gate)
    silu = gate * sig
    act = (silu * up).astype(BF)
    by_up = (by_act * silu).astype(BF)
    by_gate = (by_act * up * (sig * (1.0 + gate * (1.0 - sig)))).astype(BF)
    return act, by_gate, by_up


def write_out(accs, outs):
    @pl.when(pl.program_id(0) == pl.num_programs(0) - 1)
    def _():
        outs[0][...] = accs[0][...].astype(BF)
        outs[1][...] = accs[1][...].astype(BF)
        outs[2][...] = accs[2][...].T.astype(BF)


def zero(accs):
    @pl.when(pl.program_id(0) == 0)
    def _():
        for acc in accs:
            acc[...] = jnp.zeros_like(acc)


def top_kernel(h_ref, dy_ref, wg, wu, wd, by_h_ref, og, ou, od, ag, au, ad):
    zero((ag, au, ad))
    by_y = dy_ref[0]
    wide, scale, a = norm_of(h_ref[0])
    a_t, by_y_t = a.T, by_y.T
    by_a_g, by_a_u = jnp.zeros(a.shape[::-1], F32), jnp.zeros(a.shape[::-1], F32)
    for cols in blocks(wg.shape[1]):
        gate, up = dot(a, wg[:, cols]), dot(a, wu[:, cols])
        by_act = rounded(dot(by_y, wd[cols, :], 1, 1))
        act, by_gate, by_up = gates_back(gate, up, by_act)
        ag[:, cols] += dot(a_t, by_gate)
        au[:, cols] += dot(a_t, by_up)
        ad[:, cols] += dot(by_y_t, act)
        by_a_g += dot(wg[:, cols], by_gate, 1, 1)
        by_a_u += dot(wu[:, cols], by_up, 1, 1)
    by_a = (rounded(by_a_g) + rounded(by_a_u)).astype(BF).T.astype(F32)
    by_scale = jnp.sum(by_a * wide, -1, keepdims=True)
    by_h = by_a * scale - wide * (by_scale * scale * scale * scale / wide.shape[-1])
    by_h_ref[0] = (by_y.astype(F32) + rounded(by_h)).astype(BF)
    write_out((ag, au, ad), (og, ou, od))


def bottom_kernel(chips, x_ref, by_y_ref, gate_ref, up_ref, wd, *refs):
    top, (og, ou, od), done, (ag, au, ad) = refs[:3], refs[3:6], refs[6:9], refs[9:12]
    t, last = pl.program_id(0), pl.num_programs(0) - 1
    one = Scatter(chips, top, refs[12:])

    @pl.when(t == 0)
    def _():
        greet(one.peers)
        one.start()

    for k in range(chips - 1):
        @pl.when(t == k + 1)
        def _():
            one.step(k)

    zero((ag, au, ad))
    by_y = by_y_ref[0]
    _, _, a = norm_of(x_ref[0])
    a_t, by_y_t = a.T, by_y.T
    for cols in blocks(gate_ref.shape[1]):
        by_act = rounded(dot(by_y, wd[cols, :], 1, 1))
        act, by_gate, by_up = gates_back(gate_ref[:, cols], up_ref[:, cols], by_act)
        ag[:, cols] += dot(a_t, by_gate)
        au[:, cols] += dot(a_t, by_up)
        ad[:, cols] += dot(by_y_t, act)
    write_out((ag, au, ad), (og, ou, od))

    @pl.when(t == last)
    def _():
        one.step(chips - 1)
        for i, rows, cols, g in one.blocks():
            done[i][rows, cols] = g
        one.finish()


def tiles(width, tile=None):
    return pl.BlockSpec((tile or TILE, width), lambda t: (t, 0))


def states(width, tile=None):
    return pl.BlockSpec((1, tile or TILE, width), lambda t: (0, t, 0))


def whole(shape):
    return pl.BlockSpec(shape, lambda t: (0,) * len(shape), pipeline_mode=pl.Buffered(1))


def tiled_call(body, grid, in_specs, out_specs, out_shape, scratch, flops, name, **more):
    return pl.pallas_call(
        body, grid=(grid,), in_specs=in_specs, out_specs=out_specs, out_shape=out_shape, scratch_shapes=scratch,
        cost_estimate=pl.CostEstimate(flops=flops, bytes_accessed=flops // 1000, transcendentals=0),
        compiler_params=pltpu.CompilerParams(dimension_semantics=("arbitrary",), vmem_limit_bytes=LIMIT, **more), name=name)


def adamw(w, m, v, g):
    m = 0.9 * m + 0.1 * g
    v = 0.95 * v + 0.05 * g * g
    step = m * lax.rsqrt(v + 1e-8) + 0.1 * w
    return (w - 0.02 * step).astype(BF), m, v


def solution(mesh):
    n = mesh.shape["dp"]

    def step(x, dy, *arrays):
        weights, m, v = (arrays[i : i + 3] for i in (0, 3, 6))
        tokens, d = x.shape[1:]
        ff = weights[0].shape[2]
        grid = tokens // TILE
        flops = 2 * tokens * d * ff
        chips = n // 2
        ahead = TILE_FORWARD
        assert grid == chips and tokens == ahead * len(MOVES)
        wg0, wu0, wd0 = gather_first(weights, n)
        state = jax.ShapeDtypeStruct(x.shape, BF)
        wide = jax.ShapeDtypeStruct((tokens, ff), F32)
        across, up_and_down = (d, ff), (ff, d)
        grads = [jax.ShapeDtypeStruct(s, BF) for s in (across, across, up_and_down)]
        accs = [pltpu.VMEM(across, F32)] * 3
        ws = [whole(across), whole(across), whole(up_and_down)]
        gate, up, h, *next_w = tiled_call(
            functools.partial(forward_kernel, chips), len(MOVES), [states(d, ahead)] + ws + [whole(w.shape) for w in weights],
            [tiles(ff, ahead), tiles(ff, ahead), states(d, ahead)] + [ANY] * 3, [wide, wide, state] + gathered(weights, n), gather_sems(3, chips), 3 * flops, "forward",
            collective_id=2, has_side_effects=True,
        )(x, wg0, wu0, wd0, *weights)
        by_h, *top = tiled_call(
            top_kernel, grid, [states(d), states(d)] + ws, [states(d)] + ws, [state] + grads, accs, 8 * flops, "top"
        )(h, dy, *next_w)
        shapes = block_shapes(grads, n)
        *bottom, b0, b1, b2 = tiled_call(
            functools.partial(bottom_kernel, chips), grid, [states(d), states(d), tiles(ff), tiles(ff), ws[2]] + [ANY] * 3,
            ws + [whole(b) for b in shapes], grads + [jax.ShapeDtypeStruct(b, BF) for b in shapes],
            accs + scatter_scratch(shapes, chips), 4 * flops, "bottom", collective_id=3, has_side_effects=True,
        )(x, by_h, gate, up, wd0, *top)
        *mine, squares = scatter_last(bottom, (b0, b1, b2), n)
        count = n * sum(g.size for g in mine)
        factor = jnp.minimum(1.0, 0.5 * lax.rsqrt(squares[0, 0] / count + 1e-30))
        new = [adamw(w.astype(F32), m, v, g * factor) for w, m, v, g in zip(weights, m, v, mine, strict=True)]
        return tuple(one[which] for which in range(3) for one in new)

    states_spec, cut = P(("rep", "dp"), None, None), P(None, "dp", None)
    return jax.shard_map(
        step,
        mesh=mesh,
        in_specs=(states_spec, states_spec) + (cut,) * 9,
        out_specs=(P("rep", "dp", None),) * 9,
        check_vma=False,
    )
```

```python
import functools

import jax
import jax.numpy as jnp
from jax import lax
from jax.experimental import pallas as pl
from jax.experimental.pallas import tpu as pltpu
from jax.sharding import PartitionSpec as P

MESH = pl.DeviceIdType.MESH
BF, F32 = jnp.bfloat16, jnp.float32
ANY = pl.BlockSpec(memory_space=pl.ANY)
VM = pl.BlockSpec(memory_space=pltpu.VMEM)
TILE = 512
TILE_FORWARD = 256
COLS = 768
LIMIT = 60 * 1024 * 1024
MOVES = (5, 6, 8, 10, 11, 13, 15, 17, 18, 21, 25, 28, 31)


def dot(a, b, ca=1, cb=0):
    return lax.dot_general(a, b, (((ca,), (cb,)), ((), ())), preferred_element_type=F32)


def rounded(a):
    return a.astype(BF).astype(F32)


def norm_of(h):
    wide = h.astype(F32)
    scale = lax.rsqrt(jnp.mean(wide * wide, -1, keepdims=True) + 1e-6)
    return wide, scale, (wide * scale).astype(BF)


def place():
    me = lax.axis_index("dp")
    z, c = me // 2, me % 2
    return z, c, lambda zz, cc: {"dp": zz * 2 + cc}


def greet(peers):
    barrier = pltpu.get_barrier_semaphore()
    for p in peers:
        pl.semaphore_signal(barrier, inc=1, device_id=p, device_id_type=MESH)
    pl.semaphore_wait(barrier, len(peers))


def reach(m, chips):
    far, near = chips // 2, chips - 1 - chips // 2
    return (far, near) if m % 2 == 0 else (near, far)


class Gather:
    def __init__(self, chips, m, hops, src, out, sems):
        self.chips, self.m, self.hops, self.src, self.out = chips, m, hops, src, out
        self.ring_s, self.ring_r, self.side_s, self.side_r, self.own = sems
        self.rows = src.shape[0]
        self.z, self.c, self.dev = place()

    def at(self, zz, cc):
        return self.out.at[pl.ds(pl.multiple_of((zz * 2 + cc) * self.rows, 8), self.rows)]

    def ring(self, way, k, src=None):
        step = 1 if way == 0 else -1
        origin = (self.z - step * k + self.chips) % self.chips
        to = (self.z + step + self.chips) % self.chips
        block = self.at(origin, self.c)
        i = (0 if way == 0 else self.hops[0]) + k
        return pltpu.make_async_remote_copy(
            src_ref=block if src is None else src, dst_ref=block, send_sem=self.ring_s.at[self.m, i], recv_sem=self.ring_r.at[self.m, i],
            device_id=self.dev(to, self.c), device_id_type=MESH)

    def side(self, origin, i, src=None):
        block = self.at(origin, self.c)
        return pltpu.make_async_remote_copy(
            src_ref=block if src is None else src, dst_ref=block, send_sem=self.side_s.at[self.m, i], recv_sem=self.side_r.at[self.m, i],
            device_id=self.dev(self.z, 1 - self.c), device_id_type=MESH)

    def keep(self):
        return pltpu.make_async_copy(self.src, self.at(self.z, self.c), self.own.at[self.m])

    def start(self):
        for way in (0, 1):
            self.ring(way, 0, self.src).start()
        self.side(self.z, 0, self.src).start()
        self.keep().start()

    def step(self, k):
        for way in (0, 1):
            if k > self.hops[way]:
                continue
            self.ring(way, k - 1).wait_recv()
            if k < self.hops[way]:
                self.ring(way, k).start()
            origin = (self.z - (1 if way == 0 else -1) * k + self.chips) % self.chips
            self.side(origin, k + (0 if way == 0 else self.hops[0])).start()

    def finish(self):
        for way in (0, 1):
            for k in range(self.hops[way]):
                self.ring(way, k).wait_send()
        for i in range(self.chips):
            self.side(self.z, i).wait()
        self.keep().wait()


def gather_sems(n, chips):
    return [pltpu.SemaphoreType.DMA((n, chips - 1))] * 2 + [pltpu.SemaphoreType.DMA((n, chips))] * 2 + [pltpu.SemaphoreType.DMA((n,))]


def gathers(chips, shards, outs, sems):
    z, c, dev = place()
    peers = [dev((z + 1) % chips, c), dev((z + chips - 1) % chips, c), dev(z, 1 - c)]
    return peers, [Gather(chips, m, reach(m, chips), src, out, sems) for m, (src, out) in enumerate(zip(shards, outs, strict=True))]


def gather_kernel(chips, gate, up, *refs):
    peers, all_of = gathers(chips, (gate.at[0], up.at[0]), refs[:2], refs[2:])
    greet(peers)
    for one in all_of:
        one.start()
    for k in range(1, chips // 2 + 1):
        for one in all_of:
            one.step(k)
    for one in all_of:
        one.finish()


def gathered(weights, n):
    return [jax.ShapeDtypeStruct((w.shape[1] * n, w.shape[2]), w.dtype) for w in weights]


def gather_first(weights, n):
    chips = n // 2
    return pl.pallas_call(
        functools.partial(gather_kernel, chips),
        out_shape=gathered(weights, n),
        in_specs=[VM] * 2,
        out_specs=[ANY] * 2,
        scratch_shapes=gather_sems(2, chips),
        compiler_params=pltpu.CompilerParams(collective_id=0, has_side_effects=True),
        name="gather",
    )(*weights)


class Scatter:
    def __init__(self, chips, grads, scratch):
        self.chips, self.grads = chips, grads
        self.own, self.sides, self.slots = scratch[:3], scratch[3:6], scratch[6:12]
        self.own_sem, self.side_s, self.side_r, self.ring_s, self.ring_r = scratch[12:17]
        self.z, self.c, self.dev = place()
        self.peers = [self.dev((self.z + 1) % chips, self.c), self.dev((self.z + chips - 1) % chips, self.c), self.dev(self.z, 1 - self.c)]

    def part(self, i, zz, cc):
        rows = self.own[i].shape[-2]
        return self.grads[i].at[pl.ds(pl.multiple_of((zz * 2 + cc) * rows, 8), rows)]

    def chunk(self, way, k):
        return (self.z - 1 - k + 2 * self.chips) % self.chips if way == 0 else (self.z + 1 + k) % self.chips

    def local(self, i, zz):
        return pltpu.make_async_copy(self.part(i, zz, self.c), self.own[i].at[zz], self.own_sem.at[i, zz])

    def side(self, i, zz):
        return pltpu.make_async_remote_copy(
            src_ref=self.part(i, zz, 1 - self.c), dst_ref=self.sides[i].at[zz], send_sem=self.side_s.at[i, zz],
            recv_sem=self.side_r.at[i, zz], device_id=self.dev(self.z, 1 - self.c), device_id_type=MESH)

    def start(self):
        for k in range(self.chips):
            away = 0 if k == self.chips - 1 else -1 - k // 2 if k % 2 == 0 else 1 + k // 2
            for i, zz in ((0, self.chunk(0, k)), (1, self.chunk(1, k)), (2, (self.z + self.chips + away) % self.chips)):
                self.side(i, zz).start()
                self.local(i, zz).start()

    def ready(self, i, zz):
        self.local(i, zz).wait()
        self.side(i, zz).wait()

    def pieces(self, way):
        width, height = self.own[way].shape[-1] // 2, self.own[2].shape[-2] // 2
        every = slice(None)
        return (way, every, slice(0, width)), (way, every, slice(width, None)), (2, slice(way * height, way * height + height), every)

    def ring(self, way, j, k):
        ref = self.slots[way * 3 + j]
        to = (self.z + (1 if way == 0 else self.chips - 1)) % self.chips
        return pltpu.make_async_remote_copy(
            src_ref=ref.at[k], dst_ref=ref.at[k + 1], send_sem=self.ring_s.at[way * 3 + j, k],
            recv_sem=self.ring_r.at[way * 3 + j, k], device_id=self.dev(to, self.c), device_id_type=MESH)

    def step(self, k):
        for j in range(3):
            for way in (0, 1):
                zz = self.chunk(way, k)
                i, rows, cols = self.pieces(way)[j]
                first = 2 * k < self.chips - 1 or k == self.chips - 1 if way == 0 else 2 * k < self.chips - 2
                if j == 0 or j == 2 and first:
                    self.ready(i, zz)
                ref = self.slots[way * 3 + j]
                terms = self.own[i][zz, rows, cols].astype(F32) + self.sides[i][zz, rows, cols].astype(F32)
                if k > 0:
                    self.ring(way, j, k - 1).wait_recv()
                    terms = terms + ref[k].astype(F32)
                ref[k] = terms.astype(BF)
                if k < self.chips - 1:
                    self.ring(way, j, k).start()

    def finish(self):
        for way in (0, 1):
            for j in range(3):
                for k in range(self.chips - 1):
                    self.ring(way, j, k).wait_send()

    def blocks(self):
        return [(*piece, self.slots[way * 3 + j][self.chips - 1]) for way in (0, 1) for j, piece in enumerate(self.pieces(way))]


def block_shapes(grads, n):
    return [(g.shape[0] // n, g.shape[1]) for g in grads]


def scatter_scratch(shapes, chips):
    sem = pltpu.SemaphoreType.DMA
    across = [(h, w // 2) for h, w in shapes[:2]]
    down = (shapes[2][0] // 2, shapes[2][1])
    scratch = [pltpu.VMEM((chips, *s), BF) for s in shapes] * 2
    scratch += [pltpu.VMEM((chips, *s), BF) for s in (across[0], across[0], down, across[1], across[1], down)]
    return scratch + [sem((3, chips))] * 3 + [sem((6, chips - 1))] * 2


def scatter_kernel(chips, count, *refs):
    grads, done, outs = refs[:3], refs[3:6], refs[6:9]
    mine, sq_s, sq_r, pair, pair_sem = refs[26:]
    z, c, dev = place()
    others = [(z + k) % chips for k in range(1, chips)]
    greet([dev(o, c) for o in others] + [dev(z, 1 - c)])
    one = Scatter(chips, grads, refs[9:26])
    one.start()
    squares = jnp.zeros((), F32)
    for k in range(chips):
        one.step(k)
        if k < 3:
            g = done[k][...].astype(F32)
            outs[k][1] = g
            squares += jnp.sum(g * g)
    for i, rows, cols, g in one.blocks():
        g = g.astype(F32)
        outs[i][0, rows, cols] = g
        squares += jnp.sum(g * g)
    mine[0] = jnp.full(mine.shape[1:], squares, F32)
    copies = [
        pltpu.make_async_remote_copy(src_ref=mine.at[0], dst_ref=mine.at[k], send_sem=sq_s.at[k], recv_sem=sq_r.at[k], device_id=dev(o, c), device_id_type=MESH)
        for k, o in enumerate(others, 1)
    ]
    for copy in copies:
        copy.start()
    for copy in copies:
        copy.wait()
    pair[0] = jnp.sum(mine[...], 0)
    copy = pltpu.make_async_remote_copy(src_ref=pair.at[0], dst_ref=pair.at[1], send_sem=pair_sem.at[0], recv_sem=pair_sem.at[1], device_id=dev(z, 1 - c), device_id_type=MESH)
    copy.start()
    copy.wait()
    factor = jnp.minimum(1.0, 0.5 * lax.rsqrt((pair[0] + pair[1]) / count + 1e-30))[:1, :1]
    for out in outs:
        for l in range(out.shape[0]):
            out[l] = out[l] * factor
    one.finish()


def scatter_last(grads, done, n):
    chips = n // 2
    shapes = block_shapes(grads, n)
    sem = pltpu.SemaphoreType.DMA
    return pl.pallas_call(
        functools.partial(scatter_kernel, chips, float(2 * sum(g.size for g in grads))),
        out_shape=[jax.ShapeDtypeStruct((2, *s), F32) for s in shapes],
        in_specs=[ANY] * 3 + [VM] * 3,
        out_specs=[VM] * 3,
        scratch_shapes=scatter_scratch(shapes, chips) + [pltpu.VMEM((chips, 8, 128), F32), sem((chips,)), sem((chips,)), pltpu.VMEM((2, 8, 128), F32), sem((2,))],
        compiler_params=pltpu.CompilerParams(collective_id=1, has_side_effects=True, vmem_limit_bytes=LIMIT),
        name="scatter",
    )(*grads, *done)


def blocks(width, cols=None):
    cols = cols or COLS
    return [slice(i, i + cols) for i in range(0, width, cols)]


def forward_kernel(chips, x_ref, wg, wu, *refs):
    (gate, up, down), (gate_ref, up_ref, h_ref), outs, act, wd, copied, sems = refs[:3], refs[3:6], refs[6:10], refs[10], refs[11], refs[12], refs[13:]
    t, last = pl.program_id(0), pl.num_programs(0) - 1
    half, tile = pl.num_programs(0) // 2, x_ref.shape[1]
    peers, all_of = gathers(chips, (down.at[0], gate.at[1], up.at[1], down.at[1]), outs, sems)
    steps = range(1, chips // 2 + 1)
    moves = [(one, k) for pair in (all_of[:2], all_of[2:]) for k in steps for one in pair]

    @pl.when(t == 0)
    def _():
        greet(peers)
        all_of[0].start()
        all_of[1].start()

    for at, (one, k) in zip(MOVES, moves):
        @pl.when(t == at)
        def _():
            one.step(k)
            if k == len(steps) - 1 and one in all_of[:2]:
                all_of[2 + all_of.index(one)].start()

    x = x_ref[0]

    @pl.when(t < half)
    def _():
        _, _, a = norm_of(x)
        gate, up = dot(a, wg[...]), dot(a, wu[...])
        gate_ref[...], up_ref[...] = gate, up
        act[pl.ds(pl.multiple_of(t * tile, tile), tile)] = (gate * jax.nn.sigmoid(gate) * up).astype(BF)

    @pl.when(t == half)
    def _():
        all_of[0].finish()
        copy = pltpu.make_async_copy(outs[0], wd, copied)
        copy.start()
        copy.wait()

    @pl.when(t >= half)
    def _():
        down = dot(act[pl.ds(pl.multiple_of((t - half) * tile, tile), tile)], wd[...])
        h_ref[0] = (x.astype(F32) + rounded(down)).astype(BF)

    @pl.when(t == last)
    def _():
        for one, k in moves[len(MOVES):]:
            one.step(k)
        for one in all_of[1:]:
            one.finish()


def gates_back(gate, up, by_act):
    sig = jax.nn.sigmoid(gate)
    silu = gate * sig
    act = (silu * up).astype(BF)
    by_up = (by_act * silu).astype(BF)
    by_gate = (by_act * up * (sig * (1.0 + gate * (1.0 - sig)))).astype(BF)
    return act, by_gate, by_up


def write_out(accs, outs):
    @pl.when(pl.program_id(0) == pl.num_programs(0) - 1)
    def _():
        outs[0][...] = accs[0][...].astype(BF)
        outs[1][...] = accs[1][...].astype(BF)
        outs[2][...] = accs[2][...].T.astype(BF)


def zero(accs):
    @pl.when(pl.program_id(0) == 0)
    def _():
        for acc in accs:
            acc[...] = jnp.zeros_like(acc)


def top_kernel(h_ref, dy_ref, wg, wu, wd, by_h_ref, og, ou, od, ag, au, ad):
    zero((ag, au, ad))
    by_y = dy_ref[0]
    wide, scale, a = norm_of(h_ref[0])
    a_t, by_y_t = a.T, by_y.T
    by_a_g, by_a_u = jnp.zeros(a.shape[::-1], F32), jnp.zeros(a.shape[::-1], F32)
    for cols in blocks(wg.shape[1]):
        gate, up = dot(a, wg[:, cols]), dot(a, wu[:, cols])
        by_act = rounded(dot(by_y, wd[cols, :], 1, 1))
        act, by_gate, by_up = gates_back(gate, up, by_act)
        ag[:, cols] += dot(a_t, by_gate)
        au[:, cols] += dot(a_t, by_up)
        ad[:, cols] += dot(by_y_t, act)
        by_a_g += dot(wg[:, cols], by_gate, 1, 1)
        by_a_u += dot(wu[:, cols], by_up, 1, 1)
    by_a = (rounded(by_a_g) + rounded(by_a_u)).astype(BF).T.astype(F32)
    by_scale = jnp.sum(by_a * wide, -1, keepdims=True)
    by_h = by_a * scale - wide * (by_scale * scale * scale * scale / wide.shape[-1])
    by_h_ref[0] = (by_y.astype(F32) + rounded(by_h)).astype(BF)
    write_out((ag, au, ad), (og, ou, od))


def bottom_kernel(chips, x_ref, by_y_ref, gate_ref, up_ref, wd, *refs):
    top, (og, ou, od), done, (ag, au, ad) = refs[:3], refs[3:6], refs[6:9], refs[9:12]
    t, last = pl.program_id(0), pl.num_programs(0) - 1
    one = Scatter(chips, top, refs[12:])

    @pl.when(t == 0)
    def _():
        greet(one.peers)
        one.start()

    for k in range(chips - 1):
        @pl.when(t == k + 1)
        def _():
            one.step(k)

    zero((ag, au, ad))
    by_y = by_y_ref[0]
    _, _, a = norm_of(x_ref[0])
    a_t, by_y_t = a.T, by_y.T
    for cols in blocks(gate_ref.shape[1]):
        by_act = rounded(dot(by_y, wd[cols, :], 1, 1))
        act, by_gate, by_up = gates_back(gate_ref[:, cols], up_ref[:, cols], by_act)
        ag[:, cols] += dot(a_t, by_gate)
        au[:, cols] += dot(a_t, by_up)
        ad[:, cols] += dot(by_y_t, act)
    write_out((ag, au, ad), (og, ou, od))

    @pl.when(t == last)
    def _():
        one.step(chips - 1)
        for i, rows, cols, g in one.blocks():
            done[i][rows, cols] = g
        one.finish()


def tiles(width, tile=None):
    return pl.BlockSpec((tile or TILE, width), lambda t: (t, 0))


def states(width, tile=None):
    return pl.BlockSpec((1, tile or TILE, width), lambda t: (0, t, 0))


def whole(shape):
    return pl.BlockSpec(shape, lambda t: (0,) * len(shape), pipeline_mode=pl.Buffered(1))


def tiled_call(body, grid, in_specs, out_specs, out_shape, scratch, flops, name, **more):
    return pl.pallas_call(
        body, grid=(grid,), in_specs=in_specs, out_specs=out_specs, out_shape=out_shape, scratch_shapes=scratch,
        cost_estimate=pl.CostEstimate(flops=flops, bytes_accessed=flops // 1000, transcendentals=0),
        compiler_params=pltpu.CompilerParams(dimension_semantics=("arbitrary",), vmem_limit_bytes=LIMIT, **more), name=name)


def adamw(w, m, v, g):
    m = 0.9 * m + 0.1 * g
    v = 0.95 * v + 0.05 * g * g
    step = m * lax.rsqrt(v + 1e-8) + 0.1 * w
    return (w - 0.02 * step).astype(BF), m, v


def solution(mesh):
    n = mesh.shape["dp"]

    def step(x, dy, *arrays):
        weights, m, v = (arrays[i : i + 3] for i in (0, 3, 6))
        tokens, d = x.shape[1:]
        ff = weights[0].shape[2]
        grid = tokens // TILE
        flops = 2 * tokens * d * ff
        chips = n // 2
        ahead = TILE_FORWARD
        half = tokens // ahead
        assert grid == chips and MOVES[-1] < 2 * half
        wg0, wu0 = gather_first(weights[:2], n)
        state = jax.ShapeDtypeStruct(x.shape, BF)
        wide = jax.ShapeDtypeStruct((tokens, ff), F32)
        across, up_and_down = (d, ff), (ff, d)
        grads = [jax.ShapeDtypeStruct(s, BF) for s in (across, across, up_and_down)]
        accs = [pltpu.VMEM(across, F32)] * 3
        ws = [whole(across), whole(across), whole(up_and_down)]
        ones = pl.BlockSpec((ahead, ff), lambda t: (t - t // half * (t - half + 1), 0))
        gate, up, h, wd0, *next_w = tiled_call(
            functools.partial(forward_kernel, chips), 2 * half,
            [pl.BlockSpec((1, ahead, d), lambda t: (0, t % half, 0)), ws[0], ws[1]] + [whole(w.shape) for w in weights],
            [ones, ones, pl.BlockSpec((1, ahead, d), lambda t: (0, t // half * (t - half), 0))] + [ANY] * 4,
            [wide, wide, state] + gathered((weights[2], *weights), n),
            [pltpu.VMEM((tokens, ff), BF), pltpu.VMEM(up_and_down, BF), pltpu.SemaphoreType.DMA(())] + gather_sems(4, chips), 3 * flops, "forward",
            collective_id=2, has_side_effects=True,
        )(x, wg0, wu0, *weights)
        by_h, *top = tiled_call(
            top_kernel, grid, [states(d), states(d)] + ws, [states(d)] + ws, [state] + grads, accs, 8 * flops, "top"
        )(h, dy, *next_w)
        shapes = block_shapes(grads, n)
        *bottom, b0, b1, b2 = tiled_call(
            functools.partial(bottom_kernel, chips), grid, [states(d), states(d), tiles(ff), tiles(ff), ws[2]] + [ANY] * 3,
            ws + [whole(b) for b in shapes], grads + [jax.ShapeDtypeStruct(b, BF) for b in shapes],
            accs + scatter_scratch(shapes, chips), 4 * flops, "bottom", collective_id=3, has_side_effects=True,
        )(x, by_h, gate, up, wd0, *top)
        mine = scatter_last(bottom, (b0, b1, b2), n)
        new = [adamw(w.astype(F32), m, v, g) for w, m, v, g in zip(weights, m, v, mine, strict=True)]
        return tuple(one[which] for which in range(3) for one in new)

    states_spec, cut = P(("rep", "dp"), None, None), P(None, "dp", None)
    return jax.shard_map(
        step,
        mesh=mesh,
        in_specs=(states_spec, states_spec) + (cut,) * 9,
        out_specs=(P("rep", "dp", None),) * 9,
        check_vma=False,
    )
```

```python
import functools

import jax
import jax.numpy as jnp
from jax import lax
from jax.experimental import pallas as pl
from jax.experimental.pallas import tpu as pltpu
from jax.sharding import PartitionSpec as P

MESH = pl.DeviceIdType.MESH
BF, F32 = jnp.bfloat16, jnp.float32
ANY = pl.BlockSpec(memory_space=pl.ANY)
VM = pl.BlockSpec(memory_space=pltpu.VMEM)
TILE = 512
TILE_FORWARD = 256
COLS = 768
LIMIT = 60 * 1024 * 1024
MOVES = (0, 0, 0, 1, 2, 3, 3, 4, 5, 6, 7, 7, 8, 9, 10, 11)


def dot(a, b, ca=1, cb=0):
    return lax.dot_general(a, b, (((ca,), (cb,)), ((), ())), preferred_element_type=F32)


def rounded(a):
    return a.astype(BF).astype(F32)


def norm_of(h):
    wide = h.astype(F32)
    scale = lax.rsqrt(jnp.mean(wide * wide, -1, keepdims=True) + 1e-6)
    return wide, scale, (wide * scale).astype(BF)


def place():
    me = lax.axis_index("dp")
    z, c = me // 2, me % 2
    return z, c, lambda zz, cc: {"dp": zz * 2 + cc}


def greet(peers):
    barrier = pltpu.get_barrier_semaphore()
    for p in peers:
        pl.semaphore_signal(barrier, inc=1, device_id=p, device_id_type=MESH)
    pl.semaphore_wait(barrier, len(peers))


def reach(m, chips):
    far, near = chips // 2, chips - 1 - chips // 2
    return (far, near) if m % 2 == 0 else (near, far)


class Gather:
    def __init__(self, chips, m, hops, src, out, sems):
        self.chips, self.m, self.hops, self.src, self.out = chips, m, hops, src, out
        self.ring_s, self.ring_r, self.side_s, self.side_r, self.own = sems
        self.rows = src.shape[0]
        self.z, self.c, self.dev = place()

    def at(self, zz, cc):
        return self.out.at[pl.ds(pl.multiple_of((zz * 2 + cc) * self.rows, 8), self.rows)]

    def ring(self, way, k, src=None):
        step = 1 if way == 0 else -1
        origin = (self.z - step * k + self.chips) % self.chips
        to = (self.z + step + self.chips) % self.chips
        block = self.at(origin, self.c)
        i = (0 if way == 0 else self.hops[0]) + k
        return pltpu.make_async_remote_copy(
            src_ref=block if src is None else src, dst_ref=block, send_sem=self.ring_s.at[self.m, i], recv_sem=self.ring_r.at[self.m, i],
            device_id=self.dev(to, self.c), device_id_type=MESH)

    def side(self, origin, i, src=None):
        block = self.at(origin, self.c)
        return pltpu.make_async_remote_copy(
            src_ref=block if src is None else src, dst_ref=block, send_sem=self.side_s.at[self.m, i], recv_sem=self.side_r.at[self.m, i],
            device_id=self.dev(self.z, 1 - self.c), device_id_type=MESH)

    def keep(self):
        return pltpu.make_async_copy(self.src, self.at(self.z, self.c), self.own.at[self.m])

    def start(self):
        for way in (0, 1):
            self.ring(way, 0, self.src).start()
        self.side(self.z, 0, self.src).start()
        self.keep().start()

    def step(self, k):
        for way in (0, 1):
            if k > self.hops[way]:
                continue
            self.ring(way, k - 1).wait_recv()
            if k < self.hops[way]:
                self.ring(way, k).start()
            origin = (self.z - (1 if way == 0 else -1) * k + self.chips) % self.chips
            self.side(origin, k + (0 if way == 0 else self.hops[0])).start()

    def finish(self):
        for way in (0, 1):
            for k in range(self.hops[way]):
                self.ring(way, k).wait_send()
        for i in range(self.chips):
            self.side(self.z, i).wait()
        self.keep().wait()


def gather_sems(n, chips):
    return [pltpu.SemaphoreType.DMA((n, chips - 1))] * 2 + [pltpu.SemaphoreType.DMA((n, chips))] * 2 + [pltpu.SemaphoreType.DMA((n,))]


def gathers(chips, layer, shards, outs, sems):
    z, c, dev = place()
    peers = [dev((z + 1) % chips, c), dev((z + chips - 1) % chips, c), dev(z, 1 - c)]
    return peers, [Gather(chips, i, reach(i + layer, chips), shards[i].at[layer], outs[i], sems) for i in range(3)]


def gather_kernel(chips, *refs):
    peers, all_of = gathers(chips, 0, refs[:3], refs[3:6], refs[6:])
    greet(peers)
    for one in all_of:
        one.start()
    for k in range(1, chips // 2 + 1):
        for one in all_of:
            one.step(k)
    for one in all_of:
        one.finish()


def gathered(weights, n):
    return [jax.ShapeDtypeStruct((w.shape[1] * n, w.shape[2]), w.dtype) for w in weights]


def gather_first(weights, n):
    chips = n // 2
    return pl.pallas_call(
        functools.partial(gather_kernel, chips),
        out_shape=gathered(weights, n),
        in_specs=[VM] * 3,
        out_specs=[ANY] * 3,
        scratch_shapes=gather_sems(3, chips),
        compiler_params=pltpu.CompilerParams(collective_id=0, has_side_effects=True),
        name="gather",
    )(*weights)


class Scatter:
    def __init__(self, chips, grads, scratch):
        self.chips, self.grads = chips, grads
        self.own, self.sides, self.slots = scratch[:3], scratch[3:6], scratch[6:12]
        self.own_sem, self.side_s, self.side_r, self.ring_s, self.ring_r = scratch[12:17]
        self.z, self.c, self.dev = place()
        self.peers = [self.dev((self.z + 1) % chips, self.c), self.dev((self.z + chips - 1) % chips, self.c), self.dev(self.z, 1 - self.c)]

    def part(self, i, zz, cc):
        rows = self.own[i].shape[-2]
        return self.grads[i].at[pl.ds(pl.multiple_of((zz * 2 + cc) * rows, 8), rows)]

    def chunk(self, way, k):
        return (self.z - 1 - k + 2 * self.chips) % self.chips if way == 0 else (self.z + 1 + k) % self.chips

    def local(self, i, zz):
        return pltpu.make_async_copy(self.part(i, zz, self.c), self.own[i].at[zz], self.own_sem.at[i, zz])

    def side(self, i, zz):
        return pltpu.make_async_remote_copy(
            src_ref=self.part(i, zz, 1 - self.c), dst_ref=self.sides[i].at[zz], send_sem=self.side_s.at[i, zz],
            recv_sem=self.side_r.at[i, zz], device_id=self.dev(self.z, 1 - self.c), device_id_type=MESH)

    def start(self):
        for k in range(self.chips):
            away = 0 if k == self.chips - 1 else -1 - k // 2 if k % 2 == 0 else 1 + k // 2
            for i, zz in ((0, self.chunk(0, k)), (1, self.chunk(1, k)), (2, (self.z + self.chips + away) % self.chips)):
                self.side(i, zz).start()
                self.local(i, zz).start()

    def ready(self, i, zz):
        self.local(i, zz).wait()
        self.side(i, zz).wait()

    def pieces(self, way):
        width, height = self.own[way].shape[-1] // 2, self.own[2].shape[-2] // 2
        every = slice(None)
        return (way, every, slice(0, width)), (way, every, slice(width, None)), (2, slice(way * height, way * height + height), every)

    def ring(self, way, j, k):
        ref = self.slots[way * 3 + j]
        to = (self.z + (1 if way == 0 else self.chips - 1)) % self.chips
        return pltpu.make_async_remote_copy(
            src_ref=ref.at[k], dst_ref=ref.at[k + 1], send_sem=self.ring_s.at[way * 3 + j, k],
            recv_sem=self.ring_r.at[way * 3 + j, k], device_id=self.dev(to, self.c), device_id_type=MESH)

    def step(self, k):
        for j in range(3):
            for way in (0, 1):
                zz = self.chunk(way, k)
                i, rows, cols = self.pieces(way)[j]
                first = 2 * k < self.chips - 1 or k == self.chips - 1 if way == 0 else 2 * k < self.chips - 2
                if j == 0 or j == 2 and first:
                    self.ready(i, zz)
                ref = self.slots[way * 3 + j]
                terms = self.own[i][zz, rows, cols].astype(F32) + self.sides[i][zz, rows, cols].astype(F32)
                if k > 0:
                    self.ring(way, j, k - 1).wait_recv()
                    terms = terms + ref[k].astype(F32)
                ref[k] = terms.astype(BF)
                if k < self.chips - 1:
                    self.ring(way, j, k).start()

    def finish(self):
        for way in (0, 1):
            for j in range(3):
                for k in range(self.chips - 1):
                    self.ring(way, j, k).wait_send()

    def blocks(self):
        return [(*piece, self.slots[way * 3 + j][self.chips - 1]) for way in (0, 1) for j, piece in enumerate(self.pieces(way))]


def block_shapes(grads, n):
    return [(g.shape[0] // n, g.shape[1]) for g in grads]


def scatter_scratch(shapes, chips):
    sem = pltpu.SemaphoreType.DMA
    across = [(h, w // 2) for h, w in shapes[:2]]
    down = (shapes[2][0] // 2, shapes[2][1])
    scratch = [pltpu.VMEM((chips, *s), BF) for s in shapes] * 2
    scratch += [pltpu.VMEM((chips, *s), BF) for s in (across[0], across[0], down, across[1], across[1], down)]
    return scratch + [sem((3, chips))] * 3 + [sem((6, chips - 1))] * 2


def scatter_kernel(chips, count, *refs):
    grads, done, outs = refs[:3], refs[3:6], refs[6:9]
    mine, sq_s, sq_r, pair, pair_sem = refs[26:]
    z, c, dev = place()
    others = [(z + k) % chips for k in range(1, chips)]
    greet([dev(o, c) for o in others] + [dev(z, 1 - c)])
    one = Scatter(chips, grads, refs[9:26])
    one.start()
    squares = jnp.zeros((), F32)
    for k in range(chips):
        one.step(k)
        if k < 3:
            g = done[k][...].astype(F32)
            outs[k][1] = g
            squares += jnp.sum(g * g)
    for i, rows, cols, g in one.blocks():
        g = g.astype(F32)
        outs[i][0, rows, cols] = g
        squares += jnp.sum(g * g)
    mine[0] = jnp.full(mine.shape[1:], squares, F32)
    copies = [
        pltpu.make_async_remote_copy(src_ref=mine.at[0], dst_ref=mine.at[k], send_sem=sq_s.at[k], recv_sem=sq_r.at[k], device_id=dev(o, c), device_id_type=MESH)
        for k, o in enumerate(others, 1)
    ]
    for copy in copies:
        copy.start()
    for copy in copies:
        copy.wait()
    pair[0] = jnp.sum(mine[...], 0)
    copy = pltpu.make_async_remote_copy(src_ref=pair.at[0], dst_ref=pair.at[1], send_sem=pair_sem.at[0], recv_sem=pair_sem.at[1], device_id=dev(z, 1 - c), device_id_type=MESH)
    copy.start()
    copy.wait()
    factor = jnp.minimum(1.0, 0.5 * lax.rsqrt((pair[0] + pair[1]) / count + 1e-30))[:1, :1]
    for out in outs:
        for l in range(out.shape[0]):
            out[l] = out[l] * factor
    one.finish()


def scatter_last(grads, done, n):
    chips = n // 2
    shapes = block_shapes(grads, n)
    sem = pltpu.SemaphoreType.DMA
    return pl.pallas_call(
        functools.partial(scatter_kernel, chips, float(2 * sum(g.size for g in grads))),
        out_shape=[jax.ShapeDtypeStruct((2, *s), F32) for s in shapes],
        in_specs=[ANY] * 3 + [VM] * 3,
        out_specs=[VM] * 3,
        scratch_shapes=scatter_scratch(shapes, chips) + [pltpu.VMEM((chips, 8, 128), F32), sem((chips,)), sem((chips,)), pltpu.VMEM((2, 8, 128), F32), sem((2,))],
        compiler_params=pltpu.CompilerParams(collective_id=1, has_side_effects=True, vmem_limit_bytes=LIMIT),
        name="scatter",
    )(*grads, *done)


def blocks(width, cols=None):
    cols = cols or COLS
    return [slice(i, i + cols) for i in range(0, width, cols)]


def forward_kernel(chips, x_ref, wg, wu, wd, *refs):
    shards, (gate_ref, up_ref, h_ref), outs, sems = refs[:3], refs[3:6], refs[6:9], refs[9:]
    t, last = pl.program_id(0), pl.num_programs(0) - 1
    peers, all_of = gathers(chips, 1, shards, outs, sems)
    moves = [(one, k) for k in range(1, chips // 2 + 1) for one in all_of]

    @pl.when(t == 0)
    def _():
        greet(peers)
        for one in all_of:
            one.start()

    for at, (begin, end) in enumerate(zip(MOVES, MOVES[1:]), 1):
        @pl.when(t == at)
        def _():
            for one, k in moves[begin:end]:
                one.step(k)

    x = x_ref[0]
    _, _, a = norm_of(x)
    down = jnp.zeros(x.shape, F32)
    for cols in blocks(wg.shape[1], wg.shape[1]):
        gate, up = dot(a, wg[:, cols]), dot(a, wu[:, cols])
        gate_ref[:, cols], up_ref[:, cols] = gate, up
        act = (gate * jax.nn.sigmoid(gate) * up).astype(BF)
        down += dot(act, wd[cols, :])
    h_ref[0] = (x.astype(F32) + rounded(down)).astype(BF)

    @pl.when(t == last)
    def _():
        for one, k in moves[MOVES[-1]:]:
            one.step(k)
        for one in all_of:
            one.finish()


def gates_back(gate, up, by_act):
    sig = jax.nn.sigmoid(gate)
    silu = gate * sig
    act = (silu * up).astype(BF)
    by_up = (by_act * silu).astype(BF)
    by_gate = (by_act * up * (sig * (1.0 + gate * (1.0 - sig)))).astype(BF)
    return act, by_gate, by_up


def write_out(accs, outs):
    @pl.when(pl.program_id(0) == pl.num_programs(0) - 1)
    def _():
        outs[0][...] = accs[0][...].astype(BF)
        outs[1][...] = accs[1][...].astype(BF)
        outs[2][...] = accs[2][...].T.astype(BF)


def zero(accs):
    @pl.when(pl.program_id(0) == 0)
    def _():
        for acc in accs:
            acc[...] = jnp.zeros_like(acc)


def top_kernel(h_ref, dy_ref, wg, wu, wd, by_h_ref, og, ou, od, ag, au, ad):
    zero((ag, au, ad))
    by_y = dy_ref[0]
    wide, scale, a = norm_of(h_ref[0])
    a_t, by_y_t = a.T, by_y.T
    by_a_g, by_a_u = jnp.zeros(a.shape[::-1], F32), jnp.zeros(a.shape[::-1], F32)
    for cols in blocks(wg.shape[1]):
        gate, up = dot(a, wg[:, cols]), dot(a, wu[:, cols])
        by_act = rounded(dot(by_y, wd[cols, :], 1, 1))
        act, by_gate, by_up = gates_back(gate, up, by_act)
        ag[:, cols] += dot(a_t, by_gate)
        au[:, cols] += dot(a_t, by_up)
        ad[:, cols] += dot(by_y_t, act)
        by_a_g += dot(wg[:, cols], by_gate, 1, 1)
        by_a_u += dot(wu[:, cols], by_up, 1, 1)
    by_a = (rounded(by_a_g) + rounded(by_a_u)).astype(BF).T.astype(F32)
    by_scale = jnp.sum(by_a * wide, -1, keepdims=True)
    by_h = by_a * scale - wide * (by_scale * scale * scale * scale / wide.shape[-1])
    by_h_ref[0] = (by_y.astype(F32) + rounded(by_h)).astype(BF)
    write_out((ag, au, ad), (og, ou, od))


def bottom_kernel(chips, x_ref, by_y_ref, gate_ref, up_ref, wd, *refs):
    top, (og, ou, od), done, (ag, au, ad) = refs[:3], refs[3:6], refs[6:9], refs[9:12]
    t, last = pl.program_id(0), pl.num_programs(0) - 1
    one = Scatter(chips, top, refs[12:])

    @pl.when(t == 0)
    def _():
        greet(one.peers)
        one.start()

    for k in range(chips - 1):
        @pl.when(t == k + 1)
        def _():
            one.step(k)

    zero((ag, au, ad))
    by_y = by_y_ref[0]
    _, _, a = norm_of(x_ref[0])
    a_t, by_y_t = a.T, by_y.T
    for cols in blocks(gate_ref.shape[1]):
        by_act = rounded(dot(by_y, wd[cols, :], 1, 1))
        act, by_gate, by_up = gates_back(gate_ref[:, cols], up_ref[:, cols], by_act)
        ag[:, cols] += dot(a_t, by_gate)
        au[:, cols] += dot(a_t, by_up)
        ad[:, cols] += dot(by_y_t, act)
    write_out((ag, au, ad), (og, ou, od))

    @pl.when(t == last)
    def _():
        one.step(chips - 1)
        for i, rows, cols, g in one.blocks():
            done[i][rows, cols] = g
        one.finish()


def tiles(width, tile=None):
    return pl.BlockSpec((tile or TILE, width), lambda t: (t, 0))


def states(width, tile=None):
    return pl.BlockSpec((1, tile or TILE, width), lambda t: (0, t, 0))


def whole(shape):
    return pl.BlockSpec(shape, lambda t: (0,) * len(shape), pipeline_mode=pl.Buffered(1))


def tiled_call(body, grid, in_specs, out_specs, out_shape, scratch, flops, name, **more):
    return pl.pallas_call(
        body, grid=(grid,), in_specs=in_specs, out_specs=out_specs, out_shape=out_shape, scratch_shapes=scratch,
        cost_estimate=pl.CostEstimate(flops=flops, bytes_accessed=flops // 1000, transcendentals=0),
        compiler_params=pltpu.CompilerParams(dimension_semantics=("arbitrary",), vmem_limit_bytes=LIMIT, **more), name=name)


def adamw(w, m, v, g):
    m = 0.9 * m + 0.1 * g
    v = 0.95 * v + 0.05 * g * g
    step = m * lax.rsqrt(v + 1e-8) + 0.1 * w
    return (w - 0.02 * step).astype(BF), m, v


def solution(mesh):
    n = mesh.shape["dp"]

    def step(x, dy, *arrays):
        weights, m, v = (arrays[i : i + 3] for i in (0, 3, 6))
        tokens, d = x.shape[1:]
        ff = weights[0].shape[2]
        grid = tokens // TILE
        flops = 2 * tokens * d * ff
        chips = n // 2
        ahead = TILE_FORWARD
        assert grid == chips and tokens == ahead * len(MOVES)
        wg0, wu0, wd0 = gather_first(weights, n)
        state = jax.ShapeDtypeStruct(x.shape, BF)
        wide = jax.ShapeDtypeStruct((tokens, ff), F32)
        across, up_and_down = (d, ff), (ff, d)
        grads = [jax.ShapeDtypeStruct(s, BF) for s in (across, across, up_and_down)]
        accs = [pltpu.VMEM(across, F32)] * 3
        ws = [whole(across), whole(across), whole(up_and_down)]
        gate, up, h, *next_w = tiled_call(
            functools.partial(forward_kernel, chips), len(MOVES), [states(d, ahead)] + ws + [whole(w.shape) for w in weights],
            [tiles(ff, ahead), tiles(ff, ahead), states(d, ahead)] + [ANY] * 3, [wide, wide, state] + gathered(weights, n), gather_sems(3, chips), 3 * flops, "forward",
            collective_id=2, has_side_effects=True,
        )(x, wg0, wu0, wd0, *weights)
        by_h, *top = tiled_call(
            top_kernel, grid, [states(d), states(d)] + ws, [states(d)] + ws, [state] + grads, accs, 8 * flops, "top"
        )(h, dy, *next_w)
        shapes = block_shapes(grads, n)
        *bottom, b0, b1, b2 = tiled_call(
            functools.partial(bottom_kernel, chips), grid, [states(d), states(d), tiles(ff), tiles(ff), ws[2]] + [ANY] * 3,
            ws + [whole(b) for b in shapes], grads + [jax.ShapeDtypeStruct(b, BF) for b in shapes],
            accs + scatter_scratch(shapes, chips), 4 * flops, "bottom", collective_id=3, has_side_effects=True,
        )(x, by_h, gate, up, wd0, *top)
        mine = scatter_last(bottom, (b0, b1, b2), n)
        new = [adamw(w.astype(F32), m, v, g) for w, m, v, g in zip(weights, m, v, mine, strict=True)]
        return tuple(one[which] for which in range(3) for one in new)

    states_spec, cut = P(("rep", "dp"), None, None), P(None, "dp", None)
    return jax.shard_map(
        step,
        mesh=mesh,
        in_specs=(states_spec, states_spec) + (cut,) * 9,
        out_specs=(P("rep", "dp", None),) * 9,
        check_vma=False,
    )
```
